16 devices in a mesh: data: 4 (over z, y), expert: 4 (over x, core).
Axes of the slice: x: 2, y: 2, z: 2, core: 2. Of those that a mesh axis runs over, the one named last changes fastest.
Arguments:
- x: bfloat16 [4096, 2048], P(('data', 'expert')), parts along dimension 0
- idx: int32 [4096, 5], P(('data', 'expert')), parts along dimension 0
- g: float32 [4096, 5], P(('data', 'expert')), parts along dimension 0
- hot_tok: int32 [4096], P(('data', 'expert')), parts along dimension 0
- hot_g: float32 [4096], P(('data', 'expert')), parts along dimension 0
- ln1: float32 [2048], replicated
- wq: bfloat16 [2048, 16, 128], replicated
- wk: bfloat16 [2048, 16, 128], replicated
- wv: bfloat16 [2048, 16, 128], replicated
- wo: bfloat16 [16, 128, 2048], replicated
- ln2: float32 [2048], replicated
- w1: bfloat16 [64, 2048, 1408], P('expert')
- w3: bfloat16 [64, 2048, 1408], P('expert')
- w2: bfloat16 [64, 1408, 2048], P('expert')
Outputs:
- output: bfloat16 [4096, 2048], P(('data', 'expert')), parts along dimension 0
There are 4 independent parts. The reference program is written for one: setup_inputs(seed, part) draws one part's arguments, and reference() takes and returns one part's arrays. A program takes and returns all parts, laid end to end along the dimension named above; an argument that names none is the same for every part.
All inputs are finite; a program needn't handle non-finite values.
Results may differ from the reference program's by a relative error of at most 0.0105217.
Values are sent between devices in bfloat16 or wider.
A program may use at most 1.25 GiB of HBM per device.

```python
import jax
import jax.numpy as jnp
from jax import lax

D = 2048
FF = 1408
EXPERTS = 64
TOP = 6
HEADS = 16
HEAD = 128
TOKENS = 256
NDEV = 4
HOT = 256
HOT_ID = 1

KC = TOP - 1
C0 = (TOKENS * KC + EXPERTS - 2) // (EXPERTS - 1)
CAP = 8 * ((3 * C0 + 15) // 16)
EPS = 1e-6
ROPE_BASE = 10000.0


def _routing(key):
    k1, k2, k3, k4, k5 = jax.random.split(key, 5)
    d1, d2, d3 = jax.random.split(jax.random.fold_in(key, 7), 3)
    used = (EXPERTS - 1) - (EXPERTS - 1) // 3
    rank = jax.random.permutation(d1, TOKENS)
    c = (rank[:, None] * KC + jnp.arange(KC)[None, :]) % used
    cold = jax.random.permutation(d2, EXPERTS - 1)[c]
    idx = (cold + (cold >= HOT_ID)).astype(jnp.int32)
    start = jax.random.randint(d3, (), 0, TOKENS)
    hot_tok = ((start + jnp.arange(HOT)) % TOKENS).astype(jnp.int32)
    is_hot = jnp.zeros((TOKENS,), jnp.float32).at[hot_tok].set(1.0)
    lc = jax.random.normal(k4, (TOKENS, KC), jnp.float32)
    lh = jax.random.normal(k5, (TOKENS,), jnp.float32) + 1.0
    m = jnp.maximum(jnp.max(lc, axis=1), lh)
    ec = jnp.exp(lc - m[:, None])
    eh = jnp.exp(lh - m) * is_hot
    den = jnp.sum(ec, axis=1) + eh
    return idx, ec / den[:, None], hot_tok, (eh / den)[hot_tok]


def _normal(key, shape, fan_in):
    return (jax.random.normal(key, shape, jnp.float32) * fan_in ** -0.5).astype(jnp.bfloat16)


def _expert_weights(key, shape, fan_in):
    return lax.map(lambda k: _normal(k, shape, fan_in), jax.random.split(key, EXPERTS))


def setup_inputs(seed: int = 0, part: int = 0) -> dict:
    key = jax.random.PRNGKey(seed)
    ks = jax.random.split(key, 9)
    kx, kr = jax.random.split(jax.random.fold_in(key, part))
    x = jax.random.normal(kx, (NDEV * TOKENS, D), jnp.float32).astype(jnp.bfloat16)
    idx, g, hot_tok, hot_g = jax.vmap(_routing)(jax.random.split(kr, NDEV))
    return {
        'x': x,
        'idx': idx.reshape(NDEV * TOKENS, KC),
        'g': g.reshape(NDEV * TOKENS, KC),
        'hot_tok': hot_tok.reshape(NDEV * HOT),
        'hot_g': hot_g.reshape(NDEV * HOT),
        'ln1': jax.random.uniform(ks[0], (D,), jnp.float32, 0.5, 1.5),
        'wq': _normal(ks[1], (D, HEADS, HEAD), D),
        'wk': _normal(ks[2], (D, HEADS, HEAD), D),
        'wv': _normal(ks[3], (D, HEADS, HEAD), D),
        'wo': _normal(ks[4], (HEADS, HEAD, D), HEADS * HEAD),
        'ln2': jax.random.uniform(ks[5], (D,), jnp.float32, 0.5, 1.5),
        'w1': _expert_weights(ks[6], (D, FF), D),
        'w3': _expert_weights(ks[7], (D, FF), D),
        'w2': _expert_weights(ks[8], (FF, D), FF),
    }


def _rms(v, w):
    v = v.astype(jnp.float32)
    return (v * lax.rsqrt(jnp.mean(v * v, axis=-1, keepdims=True) + EPS) * w).astype(jnp.bfloat16)


def _rope(t):
    half = HEAD // 2
    freq = ROPE_BASE ** (-jnp.arange(half, dtype=jnp.float32) / half)
    ang = jnp.arange(TOKENS, dtype=jnp.float32)[:, None] * freq[None, :]
    cos = jnp.cos(ang)[:, None, :]
    sin = jnp.sin(ang)[:, None, :]
    t1, t2 = t[..., :half], t[..., half:]
    return jnp.concatenate([t1 * cos - t2 * sin, t2 * cos + t1 * sin], axis=-1)


def _attention(x, ln1, wq, wk, wv, wo):
    a = _rms(x, ln1).astype(jnp.float32)
    q = _rope(jnp.einsum('td,dhk->thk', a, wq.astype(jnp.float32))).astype(jnp.bfloat16)
    k = _rope(jnp.einsum('td,dhk->thk', a, wk.astype(jnp.float32))).astype(jnp.bfloat16)
    v = jnp.einsum('td,dhk->thk', a, wv.astype(jnp.float32)).astype(jnp.bfloat16)
    mask = jnp.tril(jnp.ones((TOKENS, TOKENS), bool))

    def head(qkv):
        qh, kh, vh = qkv
        s = jnp.dot(qh, kh.T, preferred_element_type=jnp.float32) * HEAD ** -0.5
        p = jax.nn.softmax(jnp.where(mask, s, -jnp.inf), axis=-1).astype(jnp.bfloat16)
        return jnp.dot(p, vh, preferred_element_type=jnp.float32).astype(jnp.bfloat16)

    o = lax.map(head, (q.transpose(1, 0, 2), k.transpose(1, 0, 2), v.transpose(1, 0, 2)))
    out = jnp.einsum('htk,hkd->td', o.astype(jnp.float32), wo.astype(jnp.float32))
    return (x.astype(jnp.float32) + out).astype(jnp.bfloat16)


def _ffn(a, w1, w3, w2):
    h1 = jnp.dot(a, w1, preferred_element_type=jnp.float32)
    h3 = jnp.dot(a, w3, preferred_element_type=jnp.float32)
    z = (jax.nn.silu(h1) * h3).astype(jnp.bfloat16)
    return jnp.dot(z, w2, preferred_element_type=jnp.float32).astype(jnp.bfloat16)


def reference(x, idx, g, hot_tok, hot_g, ln1, wq, wk, wv, wo, ln2, w1, w3, w2):
    h = lax.map(lambda s: _attention(s, ln1, wq, wk, wv, wo), x.reshape(NDEV, TOKENS, D))
    u = _rms(h.reshape(NDEV * TOKENS, D), ln2)
    e = idx.reshape(-1)
    r_all = e.shape[0]
    order = jnp.argsort(e, stable=True)
    counts = jnp.zeros((EXPERTS,), jnp.int32).at[e].add(1)
    starts = jnp.cumsum(counts) - counts
    gf = g.reshape(-1)
    rows = jnp.arange(NDEV * CAP)

    def body(y, ex):
        r = order[jnp.minimum(starts[ex] + rows, r_all - 1)]
        tok = r // KC
        out = _ffn(u[tok], w1[ex], w3[ex], w2[ex]).astype(jnp.float32)
        w = jnp.where(rows < counts[ex], gf[r], 0.0)
        return y.at[tok].add(w[:, None] * out), None

    y, _ = lax.scan(body, jnp.zeros((NDEV * TOKENS, D), jnp.float32), jnp.arange(EXPERTS))
    ht = hot_tok + jnp.repeat(jnp.arange(NDEV, dtype=jnp.int32) * TOKENS, HOT)
    ho = _ffn(u[ht], w1[HOT_ID], w3[HOT_ID], w2[HOT_ID]).astype(jnp.float32)
    y = y.at[ht].add(hot_g[:, None] * ho)
    return y.astype(jnp.bfloat16)
```

```python
import functools

import jax
import jax.numpy as jnp
from jax import lax
from jax.experimental import pallas as pl
from jax.experimental.pallas import tpu as pltpu
from jax.sharding import PartitionSpec as P

EPS = 1e-6
ROPE_BASE = 10000.0
HOT_ID = 1
SLOTS = 32
F32 = jnp.float32
BF16 = jnp.bfloat16
MESH = pl.DeviceIdType.MESH


def _rms(v, w):
    v = v.astype(F32)
    return (v * lax.rsqrt(jnp.mean(v * v, axis=-1, keepdims=True) + EPS) * w).astype(BF16)


def _rope(t):
    n_tok, _, dh = t.shape
    half = dh // 2
    freq = ROPE_BASE ** (-jnp.arange(half, dtype=F32) / half)
    ang = jnp.arange(n_tok, dtype=F32)[:, None] * freq[None, :]
    cos = jnp.cos(ang)[:, None, :]
    sin = jnp.sin(ang)[:, None, :]
    t1, t2 = t[..., :half], t[..., half:]
    return jnp.concatenate([t1 * cos - t2 * sin, t2 * cos + t1 * sin], axis=-1)


def _attention(x, ln1, wq, wk, wv, wo):
    n_tok = x.shape[0]
    dh = wq.shape[2]
    a = _rms(x, ln1)
    q = _rope(jnp.einsum('td,dhk->thk', a, wq, preferred_element_type=F32)).astype(BF16)
    k = _rope(jnp.einsum('td,dhk->thk', a, wk, preferred_element_type=F32)).astype(BF16)
    v = jnp.einsum('td,dhk->thk', a, wv, preferred_element_type=F32).astype(BF16)
    s = jnp.einsum('qhk,shk->hqs', q, k, preferred_element_type=F32) * dh ** -0.5
    mask = jnp.tril(jnp.ones((n_tok, n_tok), bool))
    p = jax.nn.softmax(jnp.where(mask[None], s, -jnp.inf), axis=-1).astype(BF16)
    o = jnp.einsum('hqs,shk->qhk', p, v, preferred_element_type=F32).astype(BF16)
    out = jnp.einsum('qhk,hkd->qd', o, wo, preferred_element_type=F32)
    return (x.astype(F32) + out).astype(BF16)


def _meta(idx, g, hot_tok, hot_g, n_exp):
    T, KC = idx.shape
    eq = idx[:, :, None] == jnp.arange(n_exp)[None, None, :]
    a = jnp.any(eq, axis=1).astype(BF16)
    low = jnp.tril(jnp.ones((T, T), BF16), -1)
    before = jnp.dot(low, a, preferred_element_type=F32)
    rank = jnp.sum(jnp.where(eq, before[:, None, :], 0.0), axis=-1)
    slot = idx.astype(F32) * SLOTS + rank
    hg = jnp.sum(jnp.where(hot_tok[:, None] == jnp.arange(T)[None, :], hot_g[:, None], 0.0), axis=0)
    return jnp.concatenate(
        [slot.T, jnp.full((8 - KC, T), -1.0, F32), g.T, hg[None], jnp.zeros((7 - KC, T), F32)], axis=0)


NU = 4
NW = 4
N2 = 8


def _moe_kernel(KC, CW, u_hbm, meta_hbm, w1, w3, w2, y_ref,
                u_all, meta, xs, zt, zh, wbuf, ob, cm, zhot, sdiag, ssib, scpt, own, rdiag, rsib, rcpt,
                in_sem, wsem, w2sem, um_send, um_recv, uc_send, uc_recv, uf_send, uf_recv, us_send, us_recv,
                dg_send, dg_recv, sb_send, sb_recv, cp_send, cp_recv):
    me = lax.axis_index('expert')
    core = me % 2
    sib = me + 1 - 2 * core
    cpt = (me + 2) % 4
    E, D, FF = w1.shape
    T = u_hbm.shape[0]
    R = E * SLOTS
    NC = D // CW
    RU = T // NU

    def start_w(i, src, odd):
        e = (i + HOT_ID) % E
        b = (2 * i + odd) % NW
        pltpu.make_async_copy(src.at[e], wbuf.at[b], wsem.at[b]).start()

    def wait_w(i, src, odd):
        b = (2 * i + odd) % NW
        pltpu.make_async_copy(src.at[0], wbuf.at[b], wsem.at[b]).wait()

    def w2_dst(t):
        sl = t % N2
        return wbuf.at[sl // 2, pl.ds(0, FF), pl.ds(pl.multiple_of((sl % 2) * CW, CW), CW)], w2sem.at[sl]

    def start_w2(t):
        dst, sem = w2_dst(t)
        e = (t % E + HOT_ID) % E
        c = t // E
        pltpu.make_async_copy(w2.at[e, :, pl.ds(pl.multiple_of(c * CW, CW), CW)], dst, sem).start()

    def wait_w2(t):
        dst, sem = w2_dst(t)
        pltpu.make_async_copy(w2.at[0, :, pl.ds(0, CW)], dst, sem).wait()

    cu = pltpu.make_async_copy(u_hbm, u_all.at[0], in_sem.at[0])
    cm_ = pltpu.make_async_copy(meta_hbm, meta.at[0], in_sem.at[1])
    cu.start()
    cm_.start()
    for i in range(NW // 2):
        start_w(i, w1, 0)
        start_w(i, w3, 1)

    barrier = pltpu.get_barrier_semaphore()
    for peer in (sib, cpt):
        pl.semaphore_signal(barrier, inc=1, device_id={'expert': peer}, device_id_type=MESH)
    cu.wait()
    cm_.wait()
    pl.semaphore_wait(barrier, 2)

    def remote(src, dst, ss, rs, peer):
        return pltpu.make_async_remote_copy(src_ref=src, dst_ref=dst, send_sem=ss, recv_sem=rs,
                                            device_id={'expert': peer}, device_id_type=MESH)

    m_sib = remote(meta.at[0], meta.at[1], um_send.at[0], um_recv.at[0], sib)
    m_cpt = remote(meta.at[0], meta.at[2], um_send.at[1], um_recv.at[1], cpt)
    m_fwd = remote(meta.at[2], meta.at[3], um_send.at[2], um_recv.at[2], sib)
    u_sib = remote(u_all.at[0], u_all.at[1], us_send, us_recv, sib)
    rows = [pl.ds(k * RU, RU) for k in range(NU)]
    u_cpt = [remote(u_all.at[0, r], u_all.at[2, r], uc_send.at[k], uc_recv.at[k], cpt) for k, r in enumerate(rows)]
    u_fwd = [remote(u_all.at[2, r], u_all.at[3, r], uf_send.at[k], uf_recv.at[k], sib) for k, r in enumerate(rows)]
    m_cpt.start()
    for c in u_cpt:
        c.start()
    m_sib.start()
    u_sib.start()

    base = (me * R).astype(F32)

    def dispatch(s):
        mt = meta[s]
        slot_iota = lax.broadcasted_iota(jnp.int32, (R, T), 0).astype(F32)
        hit = slot_iota == (mt[0:1, :] - base)
        for j in range(1, KC):
            hit = jnp.logical_or(hit, slot_iota == (mt[j:j + 1, :] - base))
        sel = jnp.where(hit, 1.0, 0.0).astype(BF16)
        for c in range(D // 512):
            cs = slice(c * 512, c * 512 + 512)
            part = jnp.dot(sel, u_all[s, :, cs], preferred_element_type=F32).astype(BF16)
            xs[:, s * SLOTS:(s + 1) * SLOTS, cs] = part.reshape(E, SLOTS, 512)
        mc = mt.T
        lane = lax.broadcasted_iota(jnp.int32, (T, R), 1).astype(F32)
        gate = jnp.zeros((T, R), F32)
        for j in range(KC):
            gate = gate + jnp.where(lane == (mc[:, j:j + 1] - base), mc[:, 8 + j:9 + j], 0.0)
        hi = gate.astype(BF16)
        r1 = gate - hi.astype(F32)
        mid = r1.astype(BF16)
        lo = (r1 - mid.astype(F32)).astype(BF16)
        cm[s, 0:T, :] = hi
        cm[s, T:2 * T, :] = mid
        cm[s, 2 * T:3 * T, :] = lo

    cols = [(0, 512), (512, 512), (1024, FF - 1024)]

    def hot_up(lo_):
        for half in range(2):
            s = lo_ + half
            for c0, cn in cols:
                a = u_all[s]
                h1 = jnp.dot(a, wbuf[0, :, c0:c0 + cn], preferred_element_type=F32)
                h3 = jnp.dot(a, wbuf[1, :, c0:c0 + cn], preferred_element_type=F32)
                zh[s, :, c0:c0 + cn] = (jax.nn.silu(h1) * h3).astype(BF16)

    def cold_up(e, b):
        for c0, cn in cols:
            a = xs[e]
            h1 = jnp.dot(a, wbuf[b, :, c0:c0 + cn], preferred_element_type=F32)
            h3 = jnp.dot(a, wbuf[b + 1, :, c0:c0 + cn], preferred_element_type=F32)
            zt[:, c0:c0 + cn] = (jax.nn.silu(h1) * h3).astype(BF16)
        xs[e, :, 0:FF] = zt[...]

    dispatch(0)
    m_sib.wait_recv()
    u_sib.wait_recv()
    dispatch(1)
    wait_w(0, w1, 0)
    wait_w(0, w3, 1)

    @pl.when(me == 0)
    def _():
        hot_up(0)

    m_cpt.wait_recv()
    m_fwd.start()
    for k in range(NU):
        u_cpt[k].wait_recv()
        u_fwd[k].start()
    dispatch(2)
    m_fwd.wait_recv()
    for k in range(NU):
        u_fwd[k].wait_recv()
    dispatch(3)

    @pl.when(me == 0)
    def _():
        hot_up(2)

    @pl.when(me != 0)
    def _():
        cold_up(HOT_ID, 0)

    start_w(NW // 2, w1, 0)
    start_w(NW // 2, w3, 1)

    def up_step(i, carry):
        e = (i + HOT_ID) % E
        b = (2 * i) % NW
        wait_w(i, w1, 0)
        wait_w(i, w3, 1)
        cold_up(e, b)

        @pl.when(i < E - NW // 2)
        def _():
            start_w(i + NW // 2, w1, 0)
            start_w(i + NW // 2, w3, 1)

        @pl.when(i >= E - NW // 2)
        def _():
            for q in range(4):
                start_w2((i - (E - NW // 2)) * 4 + q)
        return carry

    lax.fori_loop(1, E, up_step, 0)

    def chunk(c, carry):
        def down(i, carry2):
            t = c * E + i
            e = (i + HOT_ID) % E
            wait_w2(t)
            sl = t % N2
            wsl = (sl // 2, pl.ds(0, FF), pl.ds(pl.multiple_of((sl % 2) * CW, CW), CW))
            hot = jnp.logical_and(i == 0, me == 0)

            @pl.when(hot)
            def _():
                for s in range(4):
                    o = jnp.dot(zh[s], wbuf[wsl], preferred_element_type=F32).astype(BF16)
                    hg = meta[s].T[:, 13:14]
                    zhot[s] = hg * o.astype(F32)
                ob[:, HOT_ID * SLOTS:(HOT_ID + 1) * SLOTS, :] = jnp.zeros((4, SLOTS, CW), BF16)

            @pl.when(jnp.logical_not(hot))
            def _():
                o = jnp.dot(xs[e, :, 0:FF], wbuf[wsl], preferred_element_type=F32).astype(BF16)
                ob[:, pl.ds(pl.multiple_of(e * SLOTS, SLOTS), SLOTS), :] = o.reshape(4, SLOTS, CW)

            @pl.when(t + N2 < NC * E)
            def _():
                start_w2(t + N2)
            return carry2

        lax.fori_loop(0, E, down, 0)

        def combine(s):
            r = jnp.dot(cm[s], ob[s], preferred_element_type=F32)
            return (r[0:T] + r[T:2 * T]) + r[2 * T:3 * T] + zhot[s]

        p = c % 2
        d_cp = remote(sdiag.at[p], rdiag.at[c], dg_send.at[p], dg_recv.at[c], sib)
        s_cp = remote(ssib.at[p], rsib.at[c], sb_send.at[p], sb_recv.at[c], sib)
        x_cp = remote(scpt.at[c], rcpt.at[c], cp_send.at[c], cp_recv.at[c], cpt)

        @pl.when(c >= 2)
        def _():
            d_cp.wait_send()
            s_cp.wait_send()

        sdiag[p] = combine(3)
        d_cp.start()
        ssib[p] = combine(1)
        s_cp.start()
        scpt[c] = combine(2)
        own[c] = combine(0)
        d_cp.wait_recv()
        scpt[c] = scpt[c] + rdiag[c]
        x_cp.start()
        return carry

    zhot[...] = jnp.zeros_like(zhot)
    lax.fori_loop(0, NC, chunk, 0)

    for c in range(NC):
        cs = slice(c * CW, c * CW + CW)
        remote(ssib.at[0], rsib.at[c], sb_send.at[0], sb_recv.at[c], sib).wait_recv()
        remote(scpt.at[c], rcpt.at[c], cp_send.at[c], cp_recv.at[c], cpt).wait_recv()
        y_ref[:, cs] = (own[c] + rsib[c] + rcpt[c]).astype(BF16)

    m_sib.wait_send()
    m_cpt.wait_send()
    m_fwd.wait_send()
    u_sib.wait_send()
    for k in range(NU):
        u_cpt[k].wait_send()
        u_fwd[k].wait_send()
    for p in range(2):
        remote(sdiag.at[p], rdiag.at[p], dg_send.at[p], dg_recv.at[p], sib).wait_send()
        remote(ssib.at[p], rsib.at[p], sb_send.at[p], sb_recv.at[p], sib).wait_send()
    for c in range(NC):
        remote(scpt.at[c], rcpt.at[c], cp_send.at[c], cp_recv.at[c], cpt).wait_send()


def _moe(u, meta, w1, w3, w2, KC):
    T, D = u.shape
    E, _, FF = w1.shape
    CW = 512
    NC = D // CW
    R = E * SLOTS
    dma = pltpu.SemaphoreType.DMA
    any_spec = pl.BlockSpec(memory_space=pl.ANY)
    part = pltpu.VMEM((NC, T, CW), F32)
    flops = 6 * D * FF * (E * 4 * SLOTS + T)
    return pl.pallas_call(
        functools.partial(_moe_kernel, KC, CW),
        out_shape=jax.ShapeDtypeStruct((T, D), BF16),
        in_specs=[any_spec] * 5,
        out_specs=pl.BlockSpec(memory_space=pltpu.VMEM),
        scratch_shapes=[
            pltpu.VMEM((4, T, D), BF16),
            pltpu.VMEM((4, 16, T), F32),
            pltpu.VMEM((E, 4 * SLOTS, D), BF16),
            pltpu.VMEM((4 * SLOTS, FF), BF16),
            pltpu.VMEM((4, T, FF), BF16),
            pltpu.VMEM((NW, D, FF), BF16),
            pltpu.VMEM((4, R, CW), BF16),
            pltpu.VMEM((4, 3 * T, R), BF16),
            pltpu.VMEM((4, T, CW), F32),
            pltpu.VMEM((2, T, CW), F32),
            pltpu.VMEM((2, T, CW), F32),
            part, part, part, part, part,
            dma((2,)), dma((NW,)), dma((N2,)),
            dma((3,)), dma((3,)),
            dma((NU,)), dma((NU,)), dma((NU,)), dma((NU,)),
            dma, dma,
            dma((2,)), dma((NC,)), dma((2,)), dma((NC,)), dma((NC,)), dma((NC,)),
        ],
        compiler_params=pltpu.CompilerParams(
            collective_id=0, has_side_effects=True, vmem_limit_bytes=67000000),
        cost_estimate=pl.CostEstimate(flops=flops, bytes_accessed=6 * E * D * FF, transcendentals=0),
        name='moe',
    )(u, meta, w1, w3, w2)


def solution(mesh):
    def local(x, idx, g, hot_tok, hot_g, ln1, wq, wk, wv, wo, ln2, w1, w3, w2):
        n_exp = w1.shape[0] * mesh.shape['expert']
        meta = _meta(idx, g, hot_tok, hot_g, n_exp)
        u = _rms(_attention(x, ln1, wq, wk, wv, wo), ln2)
        return _moe(u, meta, w1, w3, w2, idx.shape[1])

    tk = ('data', 'expert')
    rep3 = P(None, None, None)
    exp3 = P('expert', None, None)
    return jax.shard_map(
        local, mesh=mesh,
        in_specs=(P(tk, None), P(tk, None), P(tk, None), P(tk), P(tk), P(None),
                  rep3, rep3, rep3, rep3, P(None), exp3, exp3, exp3),
        out_specs=P(tk, None), check_vma=False)
```

```python
import functools

import jax
import jax.numpy as jnp
import numpy as np
from jax import lax
from jax.experimental import pallas as pl
from jax.experimental.pallas import tpu as pltpu
from jax.sharding import PartitionSpec as P

EPS = 1e-6
ROPE_BASE = 10000.0
HOT_ID = 1
SLOTS = 32
F32 = jnp.float32
BF16 = jnp.bfloat16
MESH = pl.DeviceIdType.MESH


def _rms(v, w):
    v = v.astype(F32)
    return (v * lax.rsqrt(jnp.mean(v * v, axis=-1, keepdims=True) + EPS) * w).astype(BF16)


def _tables(n_tok, dh):
    half = dh // 2
    freq = np.float32(ROPE_BASE) ** (-np.arange(half, dtype=np.float32) / np.float32(half))
    ang = np.arange(n_tok, dtype=np.float32)[:, None] * freq[None, :].astype(np.float32)
    cos = np.cos(ang).astype(np.float32)
    sin = np.sin(ang).astype(np.float32)
    return np.concatenate([cos, cos], axis=1), np.concatenate([-sin, sin], axis=1)


def _meta(idx, g, hot_tok, hot_g, n_exp):
    T, KC = idx.shape
    eq = idx[:, :, None] == jnp.arange(n_exp)[None, None, :]
    a = jnp.any(eq, axis=1).astype(BF16)
    low = jnp.tril(jnp.ones((T, T), BF16), -1)
    before = jnp.dot(low, a, preferred_element_type=F32)
    rank = jnp.sum(jnp.where(eq, before[:, None, :], 0.0), axis=-1)
    slot = idx.astype(F32) * SLOTS + rank
    hg = jnp.sum(jnp.where(hot_tok[:, None] == jnp.arange(T)[None, :], hot_g[:, None], 0.0), axis=0)
    return jnp.concatenate(
        [slot.T, jnp.full((8 - KC, T), -1.0, F32), g.T, hg[None], jnp.zeros((7 - KC, T), F32)], axis=0)


NU = 4
NW = 4
N2 = 8
G2 = 4


def _moe_kernel(KC, CW, q_hbm, k_hbm, v_hbm, x_hbm, wo, cos_ref, sin_ref, ln2_ref, meta_hbm, w1, w3, w2, y_ref,
                u_all, meta, xs, zt, zh, wbuf, ob, cm, sel, zhot, sdiag, ssib, scpt, own, rdiag, rsib, rcpt,
                in_sem, q_sem, k_sem, v_sem, wsem, w2sem, um_send, um_recv, uc_send, uc_recv, uf_send, uf_recv,
                us_send, us_recv, dg_send, dg_recv, sb_send, sb_recv, cp_send, cp_recv):
    me = lax.axis_index('expert')
    core = me % 2
    sib = me + 1 - 2 * core
    cpt = (me + 2) % 4
    E, D, FF = w1.shape
    NH, T, DH = q_hbm.shape
    HT = T // 2
    R = E * SLOTS
    NC = D // CW
    RU = T // NU

    def start_w(i, src, odd):
        e = (i + HOT_ID) % E
        b = (2 * i + odd) % NW
        pltpu.make_async_copy(src.at[e], wbuf.at[b], wsem.at[b]).start()

    def wait_w(i, src, odd):
        b = (2 * i + odd) % NW
        pltpu.make_async_copy(src.at[0], wbuf.at[b], wsem.at[b]).wait()

    def w2_dst(t):
        sl = t % N2
        return wbuf.at[sl // 2, pl.ds(0, FF), pl.ds(pl.multiple_of((sl % 2) * CW, CW), CW)], w2sem.at[sl]

    def start_w2(t):
        dst, sem = w2_dst(t)
        e = (t % E + HOT_ID) % E
        c = t // E
        pltpu.make_async_copy(w2.at[e, :, pl.ds(pl.multiple_of(c * CW, CW), CW)], dst, sem).start()

    def wait_w2(t):
        dst, sem = w2_dst(t)
        pltpu.make_async_copy(w2.at[0, :, pl.ds(0, CW)], dst, sem).wait()

    HB = CW // DH

    def head_copy(src, dst, sem, h):
        c, lane = h // HB, (h % HB) * DH
        return pltpu.make_async_copy(src.at[h], dst.at[c, pl.ds(0, T), pl.ds(lane, DH)], sem.at[h])

    def head_wait(src, dst, sem, c, j):
        pltpu.make_async_copy(src.at[0], dst.at[c, pl.ds(0, T), pl.ds(j * DH, DH)], sem.at[c * HB + j]).wait()

    for h in range(NH):
        head_copy(q_hbm, own, q_sem, h).start()
        head_copy(k_hbm, scpt, k_sem, h).start()
        head_copy(v_hbm, ob, v_sem, h).start()
    cx = [pltpu.make_async_copy(x_hbm.at[pl.ds(i * HT, HT)], xs.at[2 + i], in_sem.at[i]) for i in range(2)]
    cwo = [pltpu.make_async_copy(wo.at[:, pl.ds(i * D // 2, D // 2)], wbuf.at[2 + i, :, pl.ds(0, D // 2)],
                                 in_sem.at[2 + i]) for i in range(2)]
    cm_ = pltpu.make_async_copy(meta_hbm, meta.at[0], in_sem.at[4])
    for c in cx + cwo + [cm_]:
        c.start()
    start_w(0, w1, 0)
    start_w(0, w3, 1)

    barrier = pltpu.get_barrier_semaphore()
    for peer in (sib, cpt):
        pl.semaphore_signal(barrier, inc=1, device_id={'expert': peer}, device_id_type=MESH)

    def remote(src, dst, ss, rs, peer):
        return pltpu.make_async_remote_copy(src_ref=src, dst_ref=dst, send_sem=ss, recv_sem=rs,
                                            device_id={'expert': peer}, device_id_type=MESH)

    m_sib = remote(meta.at[0], meta.at[1], um_send.at[0], um_recv.at[0], sib)
    m_cpt = remote(meta.at[0], meta.at[2], um_send.at[1], um_recv.at[1], cpt)
    m_fwd = remote(meta.at[2], meta.at[3], um_send.at[2], um_recv.at[2], sib)
    u_sib = [remote(u_all.at[0, pl.ds(i * HT, HT)], u_all.at[1, pl.ds(i * HT, HT)], us_send.at[i], us_recv.at[i], sib)
             for i in range(2)]

    def u_cpt(k):
        r = pl.ds(k * RU, RU)
        return remote(u_all.at[0, r], u_all.at[2, r], uc_send.at[k], uc_recv.at[k], cpt)

    def u_fwd(k):
        r = pl.ds(k * RU, RU)
        return remote(u_all.at[2, r], u_all.at[3, r], uf_send.at[k], uf_recv.at[k], sib)

    scale = DH ** -0.5

    def attend(half):
        r0 = half * HT
        nk = r0 + HT
        cos = cos_ref[r0:nk, :]
        sin = sin_ref[r0:nk, :]

        def rope(t):
            return (t * cos + pltpu.roll(t, DH // 2, 1) * sin).astype(BF16)

        row = lax.broadcasted_iota(jnp.int32, (HT, nk), 0) + r0
        seen = row >= lax.broadcasted_iota(jnp.int32, (HT, nk), 1)

        def heads(c, carry):
            for j in range(HB):
                ls = slice(j * DH, (j + 1) * DH)
                if half == 0:
                    head_wait(q_hbm, own, q_sem, c, j)
                    head_wait(k_hbm, scpt, k_sem, c, j)
                    head_wait(v_hbm, ob, v_sem, c, j)
            for j in range(HB):
                ls = slice(j * DH, (j + 1) * DH)
                q = rope(own[c, r0:nk, ls])
                ob[c, T + r0:T + nk, ls] = rope(scpt[c, r0:nk, ls])
                s = lax.dot_general(q, ob[c, T:T + nk, ls], (((1,), (1,)), ((), ())),
                                    preferred_element_type=F32) * scale
                s = jnp.where(seen, s, -jnp.inf)
                p = jnp.exp(s - jnp.max(s, axis=1, keepdims=True))
                p = (p * (1.0 / jnp.sum(p, axis=1, keepdims=True))).astype(BF16)
                o = jnp.dot(p, ob[c, 0:nk, ls], preferred_element_type=F32)
                xs[half, :, pl.ds(pl.multiple_of(c * CW + j * DH, DH), DH)] = o.astype(BF16)
            return carry

        lax.fori_loop(0, NH // HB, heads, 0)
        cx[half].wait()
        if half == 0:
            cwo[0].wait()
            cwo[1].wait()
        ss = jnp.zeros((HT, 1), F32)
        for n in range(NC):
            cs = slice(n * CW, (n + 1) * CW)
            wn = (n * CW) // (D // 2)
            w0 = n * CW - wn * (D // 2)
            o = jnp.dot(xs[half], wbuf[2 + wn, :, w0:w0 + CW], preferred_element_type=F32)
            h = (xs[2 + half, :, cs].astype(F32) + o).astype(BF16).astype(F32)
            zhot[n, 0:HT, :] = h
            ss = ss + jnp.sum(h * h, axis=1, keepdims=True)
        inv = lax.rsqrt(ss * (1.0 / D) + EPS)
        for n in range(NC):
            cs = slice(n * CW, (n + 1) * CW)
            u_all[0, r0:nk, cs] = (zhot[n, 0:HT, :] * inv * ln2_ref[0:1, cs]).astype(BF16)

    attend(0)
    cm_.wait()
    pl.semaphore_wait(barrier, 2)
    m_cpt.start()
    for k in range(NU // 2):
        u_cpt(k).start()
    m_sib.start()
    u_sib[0].start()
    attend(1)
    for k in range(NU // 2, NU):
        u_cpt(k).start()
    u_sib[1].start()
    start_w(1, w1, 0)
    start_w(1, w3, 1)

    base = (me * R).astype(F32)

    def select(s):
        mt = meta[s]
        slot_iota = lax.broadcasted_iota(jnp.int32, (R, T), 0).astype(F32)
        hit = slot_iota == (mt[0:1, :] - base)
        for j in range(1, KC):
            hit = jnp.logical_or(hit, slot_iota == (mt[j:j + 1, :] - base))
        sel[s] = jnp.where(hit, 1.0, 0.0).astype(BF16)
        mc = mt.T
        lane = lax.broadcasted_iota(jnp.int32, (T, R), 1).astype(F32)
        gate = jnp.zeros((T, R), F32)
        for j in range(KC):
            gate = gate + jnp.where(lane == (mc[:, j:j + 1] - base), mc[:, 8 + j:9 + j], 0.0)
        hi = gate.astype(BF16)
        r1 = gate - hi.astype(F32)
        mid = r1.astype(BF16)
        lo = (r1 - mid.astype(F32)).astype(BF16)
        cm[s, 0:T, :] = hi
        cm[s, T:2 * T, :] = mid
        cm[s, 2 * T:3 * T, :] = lo

    def dispatch(s):
        for c in range(D // 512):
            cs = slice(c * 512, c * 512 + 512)
            part = jnp.dot(sel[s], u_all[s, :, cs], preferred_element_type=F32).astype(BF16)
            xs[:, s * SLOTS:(s + 1) * SLOTS, cs] = part.reshape(E, SLOTS, 512)

    cols = [(0, 512), (512, 512), (1024, FF - 1024)]

    def hot_local(s, carry):
        for c0, cn in cols:
            a = u_all[s]
            h1 = jnp.dot(a, wbuf[0, :, c0:c0 + cn], preferred_element_type=F32)
            h3 = jnp.dot(a, wbuf[1, :, c0:c0 + cn], preferred_element_type=F32)
            zh[s, :, c0:c0 + cn] = (jax.nn.silu(h1) * h3).astype(BF16)
        return carry

    def hot_batch(k):
        r = pl.ds(pl.multiple_of(k * RU, RU), RU)
        a = jnp.concatenate([u_all[2, r, :], u_all[3, r, :]], axis=0)
        for c0, cn in cols:
            h1 = jnp.dot(a, wbuf[0, :, c0:c0 + cn], preferred_element_type=F32)
            h3 = jnp.dot(a, wbuf[1, :, c0:c0 + cn], preferred_element_type=F32)
            z = (jax.nn.silu(h1) * h3).astype(BF16)
            zh[2, r, c0:c0 + cn] = z[0:RU]
            zh[3, r, c0:c0 + cn] = z[RU:]

    def cold_up(e, b):
        for c0, cn in cols:
            a = xs[e]
            h1 = jnp.dot(a, wbuf[b, :, c0:c0 + cn], preferred_element_type=F32)
            h3 = jnp.dot(a, wbuf[b + 1, :, c0:c0 + cn], preferred_element_type=F32)
            zt[:, c0:c0 + cn] = (jax.nn.silu(h1) * h3).astype(BF16)
        xs[e, :, 0:FF] = zt[...]

    select(0)
    dispatch(0)
    m_sib.wait_recv()
    select(1)
    m_cpt.wait_recv()
    m_fwd.start()
    select(2)
    for i in range(2):
        u_sib[i].wait_recv()
    dispatch(1)
    wait_w(0, w1, 0)
    wait_w(0, w3, 1)

    @pl.when(me == 0)
    def _():
        lax.fori_loop(0, 2, hot_local, 0)

    m_fwd.wait_recv()
    select(3)
    u_cpt(0).wait_recv()
    u_fwd(0).start()

    def arrive(k, carry):
        u_cpt(k).wait_recv()
        u_fwd(k).start()
        u_fwd(k - 1).wait_recv()

        @pl.when(me == 0)
        def _():
            hot_batch(k - 1)
        return carry

    lax.fori_loop(1, NU, arrive, 0)
    dispatch(2)
    u_fwd(NU - 1).wait_recv()
    dispatch(3)

    @pl.when(me == 0)
    def _():
        hot_batch(NU - 1)

    @pl.when(me != 0)
    def _():
        cold_up(HOT_ID, 0)

    start_w(NW // 2, w1, 0)
    start_w(NW // 2, w3, 1)

    def up_step(i, carry):
        e = (i + HOT_ID) % E
        b = (2 * i) % NW
        wait_w(i, w1, 0)
        wait_w(i, w3, 1)
        cold_up(e, b)

        @pl.when(i < E - NW // 2)
        def _():
            start_w(i + NW // 2, w1, 0)
            start_w(i + NW // 2, w3, 1)

        @pl.when(i >= E - NW // 2)
        def _():
            for q in range(4):
                start_w2((i - (E - NW // 2)) * 4 + q)
        return carry

    lax.fori_loop(1, E, up_step, 0)

    def chunk(c, carry):
        def slot(t):
            sl = t % N2
            return (sl // 2, pl.ds(0, FF), pl.ds(pl.multiple_of((sl % 2) * CW, CW), CW))

        def cold_down(t):
            e = (t % E + HOT_ID) % E
            o = jnp.dot(xs[e, :, 0:FF], wbuf[slot(t)], preferred_element_type=F32).astype(BF16)
            ob[:, pl.ds(pl.multiple_of(e * SLOTS, SLOTS), SLOTS), :] = o.reshape(4, SLOTS, CW)

        def down(i, carry2):
            t0 = c * E + i * G2
            for q in range(G2):
                wait_w2(t0 + q)
            hot = jnp.logical_and(i == 0, me == 0)

            @pl.when(hot)
            def _():
                def hot_down(s, carry3):
                    o = jnp.dot(zh[s], wbuf[slot(t0)], preferred_element_type=F32).astype(BF16)
                    zhot[s] = meta[s].T[:, 13:14] * o.astype(F32)
                    return carry3

                lax.fori_loop(0, 4, hot_down, 0)
                ob[:, HOT_ID * SLOTS:(HOT_ID + 1) * SLOTS, :] = jnp.zeros((4, SLOTS, CW), BF16)

            @pl.when(jnp.logical_not(hot))
            def _():
                cold_down(t0)

            for q in range(1, G2):
                cold_down(t0 + q)

            @pl.when(t0 + N2 < NC * E)
            def _():
                for q in range(G2):
                    start_w2(t0 + N2 + q)
            return carry2

        lax.fori_loop(0, E // G2, down, 0)

        def combine(s):
            r = jnp.dot(cm[s], ob[s], preferred_element_type=F32)
            return (r[0:T] + r[T:2 * T]) + r[2 * T:3 * T] + zhot[s]

        p = c % 2
        d_cp = remote(sdiag.at[p], rdiag.at[c], dg_send.at[p], dg_recv.at[c], sib)
        s_cp = remote(ssib.at[p], rsib.at[c], sb_send.at[p], sb_recv.at[c], sib)
        x_cp = remote(scpt.at[c], rcpt.at[c], cp_send.at[c], cp_recv.at[c], cpt)

        @pl.when(c >= 2)
        def _():
            d_cp.wait_send()
            s_cp.wait_send()

        sdiag[p] = combine(3)
        d_cp.start()
        ssib[p] = combine(1)
        s_cp.start()
        scpt[c] = combine(2)
        own[c] = combine(0)
        d_cp.wait_recv()
        scpt[c] = scpt[c] + rdiag[c]
        x_cp.start()
        return carry

    zhot[...] = jnp.zeros_like(zhot)
    lax.fori_loop(0, NC, chunk, 0)

    for c in range(NC):
        cs = slice(c * CW, c * CW + CW)
        remote(ssib.at[0], rsib.at[c], sb_send.at[0], sb_recv.at[c], sib).wait_recv()
        remote(scpt.at[c], rcpt.at[c], cp_send.at[c], cp_recv.at[c], cpt).wait_recv()
        y_ref[:, cs] = (own[c] + rsib[c] + rcpt[c]).astype(BF16)

    m_sib.wait_send()
    m_cpt.wait_send()
    m_fwd.wait_send()
    for i in range(2):
        u_sib[i].wait_send()
    for k in range(NU):
        u_cpt(k).wait_send()
        u_fwd(k).wait_send()
    for p in range(2):
        remote(sdiag.at[p], rdiag.at[p], dg_send.at[p], dg_recv.at[p], sib).wait_send()
        remote(ssib.at[p], rsib.at[p], sb_send.at[p], sb_recv.at[p], sib).wait_send()
    for c in range(NC):
        remote(scpt.at[c], rcpt.at[c], cp_send.at[c], cp_recv.at[c], cpt).wait_send()


def _moe(q, k, v, x, wo, ln2, meta, w1, w3, w2, KC):
    NH, T, DH = q.shape
    D = x.shape[1]
    E, _, FF = w1.shape
    CW = 512
    NC = D // CW
    R = E * SLOTS
    dma = pltpu.SemaphoreType.DMA
    cos, sin = _tables(T, DH)
    vm = pl.BlockSpec(memory_space=pltpu.VMEM)
    any_spec = pl.BlockSpec(memory_space=pl.ANY)
    part = pltpu.VMEM((NC, T, CW), F32)
    flops = 6 * D * FF * (E * 4 * SLOTS + T)
    return pl.pallas_call(
        functools.partial(_moe_kernel, KC, CW),
        out_shape=jax.ShapeDtypeStruct((T, D), BF16),
        in_specs=[any_spec] * 5 + [vm] * 3 + [any_spec] * 4,
        out_specs=pl.BlockSpec(memory_space=pltpu.VMEM),
        scratch_shapes=[
            pltpu.VMEM((4, T, D), BF16),
            pltpu.VMEM((4, 16, T), F32),
            pltpu.VMEM((E, 4 * SLOTS, D), BF16),
            pltpu.VMEM((4 * SLOTS, FF), BF16),
            pltpu.VMEM((4, T, FF), BF16),
            pltpu.VMEM((NW, D, FF), BF16),
            pltpu.VMEM((4, R, CW), BF16),
            pltpu.VMEM((4, 3 * T, R), BF16),
            pltpu.VMEM((4, R, T), BF16),
            pltpu.VMEM((4, T, CW), F32),
            pltpu.VMEM((2, T, CW), F32),
            pltpu.VMEM((2, T, CW), F32),
            part, part, part, part, part,
            dma((5,)), dma((NH,)), dma((NH,)), dma((NH,)), dma((NW,)), dma((N2,)),
            dma((3,)), dma((3,)),
            dma((NU,)), dma((NU,)), dma((NU,)), dma((NU,)),
            dma((2,)), dma((2,)),
            dma((2,)), dma((NC,)), dma((2,)), dma((NC,)), dma((NC,)), dma((NC,)),
        ],
        compiler_params=pltpu.CompilerParams(
            collective_id=0, has_side_effects=True, vmem_limit_bytes=67000000),
        cost_estimate=pl.CostEstimate(flops=flops, bytes_accessed=6 * E * D * FF, transcendentals=0),
        name='moe',
    )(q, k, v, x, wo.reshape(D, D), jnp.asarray(cos), jnp.asarray(sin), ln2.reshape(1, D), meta, w1, w3, w2)


def solution(mesh):
    def local(x, idx, g, hot_tok, hot_g, ln1, wq, wk, wv, wo, ln2, w1, w3, w2):
        n_exp = w1.shape[0] * mesh.shape['expert']
        meta = _meta(idx, g, hot_tok, hot_g, n_exp)
        a = _rms(x, ln1)
        q = jnp.einsum('td,dhk->htk', a, wq, preferred_element_type=F32)
        k = jnp.einsum('td,dhk->htk', a, wk, preferred_element_type=F32)
        v = jnp.einsum('td,dhk->htk', a, wv, preferred_element_type=F32).astype(BF16)
        return _moe(q, k, v, x, wo, ln2, meta, w1, w3, w2, idx.shape[1])

    tk = ('data', 'expert')
    rep3 = P(None, None, None)
    exp3 = P('expert', None, None)
    return jax.shard_map(
        local, mesh=mesh,
        in_specs=(P(tk, None), P(tk, None), P(tk, None), P(tk), P(tk), P(None),
                  rep3, rep3, rep3, rep3, P(None), exp3, exp3, exp3),
        out_specs=P(tk, None), check_vma=False)
```

```python
import functools

import jax
import jax.numpy as jnp
import numpy as np
from jax import lax
from jax.experimental import pallas as pl
from jax.experimental.pallas import tpu as pltpu
from jax.sharding import PartitionSpec as P

EPS = 1e-6
ROPE_BASE = 10000.0
HOT_ID = 1
SLOTS = 32
F32 = jnp.float32
BF16 = jnp.bfloat16
MESH = pl.DeviceIdType.MESH


def _tables(n_tok, dh):
    half = dh // 2
    freq = np.float32(ROPE_BASE) ** (-np.arange(half, dtype=np.float32) / np.float32(half))
    ang = np.arange(n_tok, dtype=np.float32)[:, None] * freq[None, :].astype(np.float32)
    cos = np.cos(ang).astype(np.float32)
    sin = np.sin(ang).astype(np.float32)
    return np.concatenate([cos, cos], axis=1), np.concatenate([-sin, sin], axis=1)


def _qkv_kernel(n_exp, x_ref, ln1_ref, cos_ref, sin_ref, idx_ref, g_ref, tok_ref, hg_ref, wv, wk, wq,
                v_ref, k_ref, q_ref, meta_ref, wb, acc, ab, sem):
    T, D = x_ref.shape
    NH, _, DH = q_ref.shape
    NB, KB = wb.shape[1], wb.shape[2]
    ws = (wv, wk, wq)

    def copy(i, b):
        return pltpu.make_async_copy(ws[i].at[pl.ds(b * KB, KB)], wb.at[i, b], sem.at[i, b])

    for i in range(3):
        for b in range(NB):
            copy(i, b).start()

    ss = jnp.zeros((T, 1), F32)
    for c in range(0, D, 512):
        xc = x_ref[:, c:c + 512].astype(F32)
        ss = ss + jnp.sum(xc * xc, axis=1, keepdims=True)
    inv = lax.rsqrt(ss * (1.0 / D) + EPS)
    for c in range(0, D, 512):
        ab[:, c:c + 512] = (x_ref[:, c:c + 512].astype(F32) * inv * ln1_ref[0:1, c:c + 512]).astype(BF16)

    KC = idx_ref.shape[0]
    e_iota = lax.broadcasted_iota(jnp.int32, (n_exp, T), 0)
    hits = [e_iota == idx_ref[j:j + 1, :] for j in range(KC)]
    member = hits[0]
    for h in hits[1:]:
        member = jnp.logical_or(member, h)
    earlier = lax.broadcasted_iota(jnp.int32, (T, T), 0) < lax.broadcasted_iota(jnp.int32, (T, T), 1)
    before = jnp.dot(jnp.where(member, 1.0, 0.0).astype(BF16), jnp.where(earlier, 1.0, 0.0).astype(BF16),
                     preferred_element_type=F32)
    meta_ref[...] = jnp.full((16, T), -1.0, F32)
    for j in range(KC):
        rank = jnp.sum(jnp.where(hits[j], before, 0.0), axis=0, keepdims=True)
        meta_ref[j:j + 1, :] = idx_ref[j:j + 1, :].astype(F32) * SLOTS + rank
        meta_ref[8 + j:9 + j, :] = g_ref[j:j + 1, :]
    tok = jnp.broadcast_to(tok_ref[...].astype(F32), (8, T)).T[:, 0:1]
    hg = jnp.broadcast_to(hg_ref[...], (8, T)).T[:, 0:1]
    t_iota = lax.broadcasted_iota(jnp.int32, (T, T), 1).astype(F32)
    meta_ref[13:14, :] = jnp.sum(jnp.where(tok == t_iota, hg, 0.0), axis=0, keepdims=True)

    for i, out in enumerate((v_ref, k_ref, q_ref)):
        for b in range(NB):
            copy(i, b).wait()
            part = jnp.dot(ab[:, b * KB:(b + 1) * KB], wb[i, b].reshape(KB, D), preferred_element_type=F32)
            if b < NB - 1:
                acc[...] = part if b == 0 else acc[...] + part
                continue
            for h in range(NH):
                t = part[:, h * DH:(h + 1) * DH]
                if NB > 1:
                    t = t + acc[:, h * DH:(h + 1) * DH]
                if i > 0:
                    t = t * cos_ref[...] + pltpu.roll(t, DH // 2, 1) * sin_ref[...]
                out[h] = t.astype(BF16)


def _qkv(x, ln1, wq, wk, wv, idx, g, hot_tok, hot_g, n_exp):
    T, D = x.shape
    _, NH, DH = wq.shape
    NB = 2
    cos, sin = _tables(T, DH)
    vm = pl.BlockSpec(memory_space=pltpu.VMEM)
    any_spec = pl.BlockSpec(memory_space=pl.ANY)
    head = jax.ShapeDtypeStruct((NH, T, DH), BF16)
    return pl.pallas_call(
        functools.partial(_qkv_kernel, n_exp),
        out_shape=[head, head, head, jax.ShapeDtypeStruct((16, T), F32)],
        in_specs=[vm] * 8 + [any_spec] * 3,
        out_specs=[vm] * 4,
        scratch_shapes=[
            pltpu.VMEM((3, NB, D // NB, NH, DH), BF16),
            pltpu.VMEM((T, D), F32),
            pltpu.VMEM((T, D), BF16),
            pltpu.SemaphoreType.DMA((3, NB)),
        ],
        compiler_params=pltpu.CompilerParams(vmem_limit_bytes=60000000),
        cost_estimate=pl.CostEstimate(flops=6 * T * D * D, bytes_accessed=6 * D * D, transcendentals=0),
        name='qkv',
    )(x, ln1.reshape(1, D), jnp.asarray(cos), jnp.asarray(sin), idx.T, g.T, hot_tok.reshape(1, T),
      hot_g.reshape(1, T), wv, wk, wq)


NU = 4
NW = 4
N2 = 8
G2 = 4


def _moe_kernel(KC, CW, q_hbm, k_hbm, v_hbm, x_hbm, wo, ln2_ref, meta_hbm, w1, w3, w2, y_ref,
                u_all, meta, xs, zt, zh, wbuf, ob, cm, sel, hgc, zhot, sdiag, ssib, scpt, own, rdiag, rsib, rcpt,
                in_sem, q_sem, k_sem, v_sem, wsem, w2sem, um_send, um_recv, uc_send, uc_recv, uf_send, uf_recv,
                us_send, us_recv, dg_send, dg_recv, sb_send, sb_recv, cp_send, cp_recv):
    me = lax.axis_index('expert')
    core = me % 2
    sib = me + 1 - 2 * core
    cpt = (me + 2) % 4
    E, D, FF = w1.shape
    NH, T, DH = q_hbm.shape
    HT = T // 2
    R = E * SLOTS
    NC = D // CW
    RU = T // NU

    def start_w(i, src, odd):
        e = (i + HOT_ID) % E
        b = (2 * i + odd) % NW
        pltpu.make_async_copy(src.at[e], wbuf.at[b], wsem.at[b]).start()

    def wait_w(i, src, odd):
        b = (2 * i + odd) % NW
        pltpu.make_async_copy(src.at[0], wbuf.at[b], wsem.at[b]).wait()

    def w2_dst(t):
        sl = t % N2
        return wbuf.at[sl // 2, pl.ds(0, FF), pl.ds(pl.multiple_of((sl % 2) * CW, CW), CW)], w2sem.at[sl]

    def start_w2(t):
        dst, sem = w2_dst(t)
        e = (t % E + HOT_ID) % E
        c = t // E
        pltpu.make_async_copy(w2.at[e, :, pl.ds(pl.multiple_of(c * CW, CW), CW)], dst, sem).start()

    def wait_w2(t):
        dst, sem = w2_dst(t)
        pltpu.make_async_copy(w2.at[0, :, pl.ds(0, CW)], dst, sem).wait()

    HB = CW // DH

    bufs = ((q_hbm, zh, 0, q_sem), (k_hbm, ob, T, k_sem), (v_hbm, ob, 0, v_sem))

    def head_copy(b, h, c, j):
        src, dst, r0, sem = bufs[b]
        return pltpu.make_async_copy(src.at[h], dst.at[c, pl.ds(r0, T), pl.ds(j * DH, DH)], sem.at[c * HB + j])

    for h in range(NH):
        for b in range(3):
            head_copy(b, h, h // HB, h % HB).start()
    cx = [pltpu.make_async_copy(x_hbm.at[pl.ds(i * HT, HT)], xs.at[2 + i], in_sem.at[i]) for i in range(2)]
    cwo = [pltpu.make_async_copy(wo.at[:, pl.ds(i * D // 2, D // 2)], wbuf.at[2 + i, :, pl.ds(0, D // 2)],
                                 in_sem.at[2 + i]) for i in range(2)]
    cm_ = pltpu.make_async_copy(meta_hbm, meta.at[0], in_sem.at[4])
    for c in cx + cwo + [cm_]:
        c.start()
    start_w(0, w1, 0)
    start_w(0, w3, 1)

    barrier = pltpu.get_barrier_semaphore()
    for peer in (sib, cpt):
        pl.semaphore_signal(barrier, inc=1, device_id={'expert': peer}, device_id_type=MESH)

    def remote(src, dst, ss, rs, peer):
        return pltpu.make_async_remote_copy(src_ref=src, dst_ref=dst, send_sem=ss, recv_sem=rs,
                                            device_id={'expert': peer}, device_id_type=MESH)

    m_sib = remote(meta.at[0], meta.at[1], um_send.at[0], um_recv.at[0], sib)
    m_cpt = remote(meta.at[0], meta.at[2], um_send.at[1], um_recv.at[1], cpt)
    m_fwd = remote(meta.at[2], meta.at[3], um_send.at[2], um_recv.at[2], sib)
    u_sib = [remote(u_all.at[0, pl.ds(i * HT, HT)], u_all.at[1, pl.ds(i * HT, HT)], us_send.at[i], us_recv.at[i], sib)
             for i in range(2)]

    def u_cpt(k):
        r = pl.ds(k * RU, RU)
        return remote(u_all.at[0, r], u_all.at[2, r], uc_send.at[k], uc_recv.at[k], cpt)

    def u_fwd(k):
        r = pl.ds(k * RU, RU)
        return remote(u_all.at[2, r], u_all.at[3, r], uf_send.at[k], uf_recv.at[k], sib)

    scale = DH ** -0.5

    def attend(half):
        r0 = half * HT
        nk = r0 + HT
        row = lax.broadcasted_iota(jnp.int32, (HT, nk), 0) + r0
        seen = row >= lax.broadcasted_iota(jnp.int32, (HT, nk), 1)

        def heads(c, carry):
            if half == 0:
                for j in range(HB):
                    for b in range(3):
                        head_copy(b, 0, c, j).wait()
            lanes = [slice(j * DH, (j + 1) * DH) for j in range(HB)]
            sc = [lax.dot_general(zh[c, r0:nk, ls], ob[c, T:T + nk, ls], (((1,), (1,)), ((), ())),
                                  preferred_element_type=F32) for ls in lanes]
            sc = [jnp.where(seen, s * scale, -jnp.inf) for s in sc]
            ps = [jnp.exp(s - jnp.max(s, axis=1, keepdims=True)) for s in sc]
            ps = [(p * (1.0 / jnp.sum(p, axis=1, keepdims=True))).astype(BF16) for p in ps]
            os = [jnp.dot(p, ob[c, 0:nk, ls], preferred_element_type=F32) for p, ls in zip(ps, lanes)]
            for j in range(HB):
                xs[half, :, pl.ds(pl.multiple_of(c * CW + j * DH, DH), DH)] = os[j].astype(BF16)
            return carry

        lax.fori_loop(0, NH // HB, heads, 0)
        cx[half].wait()
        if half == 0:
            cwo[0].wait()
            cwo[1].wait()
        ss = jnp.zeros((HT, 1), F32)
        for n in range(NC):
            cs = slice(n * CW, (n + 1) * CW)
            wn = (n * CW) // (D // 2)
            w0 = n * CW - wn * (D // 2)
            o = jnp.dot(xs[half], wbuf[2 + wn, :, w0:w0 + CW], preferred_element_type=F32)
            h = (xs[2 + half, :, cs].astype(F32) + o).astype(BF16).astype(F32)
            zhot[n, 0:HT, :] = h
            ss = ss + jnp.sum(h * h, axis=1, keepdims=True)
        inv = lax.rsqrt(ss * (1.0 / D) + EPS)
        for n in range(NC):
            cs = slice(n * CW, (n + 1) * CW)
            u_all[0, r0:nk, cs] = (zhot[n, 0:HT, :] * inv * ln2_ref[0:1, cs]).astype(BF16)

    attend(0)
    cm_.wait()
    pl.semaphore_wait(barrier, 2)
    m_cpt.start()
    for k in range(NU // 2):
        u_cpt(k).start()
    m_sib.start()
    u_sib[0].start()
    attend(1)
    for k in range(NU // 2, NU):
        u_cpt(k).start()
    u_sib[1].start()
    start_w(1, w1, 0)
    start_w(1, w3, 1)

    base = (me * R).astype(F32)

    def select(s):
        mt = meta[s]
        slot_iota = lax.broadcasted_iota(jnp.int32, (R, T), 0).astype(F32)
        hit = slot_iota == (mt[0:1, :] - base)
        for j in range(1, KC):
            hit = jnp.logical_or(hit, slot_iota == (mt[j:j + 1, :] - base))
        sel[s] = jnp.where(hit, 1.0, 0.0).astype(BF16)
        mc = mt.T
        lane = lax.broadcasted_iota(jnp.int32, (T, R), 1).astype(F32)
        gate = jnp.zeros((T, R), F32)
        for j in range(KC):
            gate = gate + jnp.where(lane == (mc[:, j:j + 1] - base), mc[:, 8 + j:9 + j], 0.0)
        hi = gate.astype(BF16)
        r1 = gate - hi.astype(F32)
        mid = r1.astype(BF16)
        lo = (r1 - mid.astype(F32)).astype(BF16)
        hgc[s] = mc[:, 13:14]
        cm[s, 0:T, :] = hi
        cm[s, T:2 * T, :] = mid
        cm[s, 2 * T:3 * T, :] = lo

    def dispatch(s):
        for c in range(D // 512):
            cs = slice(c * 512, c * 512 + 512)
            part = jnp.dot(sel[s], u_all[s, :, cs], preferred_element_type=F32).astype(BF16)
            xs[:, s * SLOTS:(s + 1) * SLOTS, cs] = part.reshape(E, SLOTS, 512)

    cols = [(0, 512), (512, 512), (1024, FF - 1024)]

    def hot_local(s, carry):
        for c0, cn in cols:
            a = u_all[s]
            h1 = jnp.dot(a, wbuf[0, :, c0:c0 + cn], preferred_element_type=F32)
            h3 = jnp.dot(a, wbuf[1, :, c0:c0 + cn], preferred_element_type=F32)
            zh[s, :, c0:c0 + cn] = (jax.nn.silu(h1) * h3).astype(BF16)
        return carry

    def hot_batch(k):
        r = pl.ds(pl.multiple_of(k * RU, RU), RU)
        a = jnp.concatenate([u_all[2, r, :], u_all[3, r, :]], axis=0)
        for c0, cn in cols:
            h1 = jnp.dot(a, wbuf[0, :, c0:c0 + cn], preferred_element_type=F32)
            h3 = jnp.dot(a, wbuf[1, :, c0:c0 + cn], preferred_element_type=F32)
            z = (jax.nn.silu(h1) * h3).astype(BF16)
            zh[2, r, c0:c0 + cn] = z[0:RU]
            zh[3, r, c0:c0 + cn] = z[RU:]

    def cold_up(e, b):
        for c0, cn in cols:
            a = xs[e]
            h1 = jnp.dot(a, wbuf[b, :, c0:c0 + cn], preferred_element_type=F32)
            h3 = jnp.dot(a, wbuf[b + 1, :, c0:c0 + cn], preferred_element_type=F32)
            zt[:, c0:c0 + cn] = (jax.nn.silu(h1) * h3).astype(BF16)
        xs[e, :, 0:FF] = zt[...]

    select(0)
    dispatch(0)
    m_sib.wait_recv()
    select(1)
    m_cpt.wait_recv()
    m_fwd.start()
    select(2)
    for i in range(2):
        u_sib[i].wait_recv()
    dispatch(1)
    wait_w(0, w1, 0)
    wait_w(0, w3, 1)

    @pl.when(me == 0)
    def _():
        lax.fori_loop(0, 2, hot_local, 0)

    m_fwd.wait_recv()
    select(3)
    u_cpt(0).wait_recv()
    u_fwd(0).start()

    def arrive(k, carry):
        u_cpt(k).wait_recv()
        u_fwd(k).start()
        u_fwd(k - 1).wait_recv()

        @pl.when(me == 0)
        def _():
            hot_batch(k - 1)
        return carry

    lax.fori_loop(1, NU, arrive, 0)
    dispatch(2)
    u_fwd(NU - 1).wait_recv()
    dispatch(3)

    @pl.when(me == 0)
    def _():
        hot_batch(NU - 1)

    @pl.when(me != 0)
    def _():
        cold_up(HOT_ID, 0)

    start_w(NW // 2, w1, 0)
    start_w(NW // 2, w3, 1)

    def up_step(i, carry):
        e = (i + HOT_ID) % E
        b = (2 * i) % NW
        wait_w(i, w1, 0)
        wait_w(i, w3, 1)
        cold_up(e, b)

        @pl.when(i < E - NW // 2)
        def _():
            start_w(i + NW // 2, w1, 0)
            start_w(i + NW // 2, w3, 1)

        @pl.when(i >= E - NW // 2)
        def _():
            for q in range(4):
                start_w2((i - (E - NW // 2)) * 4 + q)
        return carry

    lax.fori_loop(1, E, up_step, 0)

    def chunk(c, carry):
        def slot(t):
            sl = t % N2
            return (sl // 2, pl.ds(0, FF), pl.ds(pl.multiple_of((sl % 2) * CW, CW), CW))

        def cold_down(t):
            e = (t % E + HOT_ID) % E
            o = jnp.dot(xs[e, :, 0:FF], wbuf[slot(t)], preferred_element_type=F32).astype(BF16)
            ob[:, pl.ds(pl.multiple_of(e * SLOTS, SLOTS), SLOTS), :] = o.reshape(4, SLOTS, CW)

        def down(i, carry2):
            t0 = c * E + i * G2
            for q in range(G2):
                wait_w2(t0 + q)
            hot = jnp.logical_and(i == 0, me == 0)

            @pl.when(hot)
            def _():
                def hot_down(s, carry3):
                    o = jnp.dot(zh[s], wbuf[slot(t0)], preferred_element_type=F32).astype(BF16)
                    zhot[s] = hgc[s] * o.astype(F32)
                    return carry3

                lax.fori_loop(0, 4, hot_down, 0)
                ob[:, HOT_ID * SLOTS:(HOT_ID + 1) * SLOTS, :] = jnp.zeros((4, SLOTS, CW), BF16)

            @pl.when(jnp.logical_not(hot))
            def _():
                cold_down(t0)

            for q in range(1, G2):
                cold_down(t0 + q)

            @pl.when(t0 + N2 < NC * E)
            def _():
                for q in range(G2):
                    start_w2(t0 + N2 + q)
            return carry2

        lax.fori_loop(0, E // G2, down, 0)

        def combine(s):
            r = jnp.dot(cm[s], ob[s], preferred_element_type=F32)
            return (r[0:T] + r[T:2 * T]) + r[2 * T:3 * T] + zhot[s]

        p = c % 2
        d_cp = remote(sdiag.at[p], rdiag.at[c], dg_send.at[p], dg_recv.at[c], sib)
        s_cp = remote(ssib.at[p], rsib.at[c], sb_send.at[p], sb_recv.at[c], sib)
        x_cp = remote(scpt.at[c], rcpt.at[c], cp_send.at[c], cp_recv.at[c], cpt)

        @pl.when(c >= 2)
        def _():
            d_cp.wait_send()
            s_cp.wait_send()

        sdiag[p] = combine(3)
        d_cp.start()
        ssib[p] = combine(1)
        s_cp.start()
        scpt[c] = combine(2)
        own[c] = combine(0)
        d_cp.wait_recv()
        scpt[c] = scpt[c] + rdiag[c]
        x_cp.start()
        return carry

    zhot[...] = jnp.zeros_like(zhot)
    lax.fori_loop(0, NC, chunk, 0)

    for c in range(NC):
        cs = slice(c * CW, c * CW + CW)
        remote(ssib.at[0], rsib.at[c], sb_send.at[0], sb_recv.at[c], sib).wait_recv()
        remote(scpt.at[c], rcpt.at[c], cp_send.at[c], cp_recv.at[c], cpt).wait_recv()
        y_ref[:, cs] = (own[c] + rsib[c] + rcpt[c]).astype(BF16)

    m_sib.wait_send()
    m_cpt.wait_send()
    m_fwd.wait_send()
    for i in range(2):
        u_sib[i].wait_send()
    for k in range(NU):
        u_cpt(k).wait_send()
        u_fwd(k).wait_send()
    for p in range(2):
        remote(sdiag.at[p], rdiag.at[p], dg_send.at[p], dg_recv.at[p], sib).wait_send()
        remote(ssib.at[p], rsib.at[p], sb_send.at[p], sb_recv.at[p], sib).wait_send()
    for c in range(NC):
        remote(scpt.at[c], rcpt.at[c], cp_send.at[c], cp_recv.at[c], cpt).wait_send()


def _moe(q, k, v, x, wo, ln2, meta, w1, w3, w2, KC):
    NH, T, DH = q.shape
    D = x.shape[1]
    E, _, FF = w1.shape
    CW = 512
    NC = D // CW
    R = E * SLOTS
    dma = pltpu.SemaphoreType.DMA
    vm = pl.BlockSpec(memory_space=pltpu.VMEM)
    any_spec = pl.BlockSpec(memory_space=pl.ANY)
    part = pltpu.VMEM((NC, T, CW), F32)
    flops = 6 * D * FF * (E * 4 * SLOTS + T)
    return pl.pallas_call(
        functools.partial(_moe_kernel, KC, CW),
        out_shape=jax.ShapeDtypeStruct((T, D), BF16),
        in_specs=[any_spec] * 5 + [vm] + [any_spec] * 4,
        out_specs=pl.BlockSpec(memory_space=pltpu.VMEM),
        scratch_shapes=[
            pltpu.VMEM((4, T, D), BF16),
            pltpu.VMEM((4, 16, T), F32),
            pltpu.VMEM((E, 4 * SLOTS, D), BF16),
            pltpu.VMEM((4 * SLOTS, FF), BF16),
            pltpu.VMEM((4, T, FF), BF16),
            pltpu.VMEM((NW, D, FF), BF16),
            pltpu.VMEM((4, R, CW), BF16),
            pltpu.VMEM((4, 3 * T, R), BF16),
            pltpu.VMEM((4, R, T), BF16),
            pltpu.VMEM((4, T, 1), F32),
            pltpu.VMEM((4, T, CW), F32),
            pltpu.VMEM((2, T, CW), F32),
            pltpu.VMEM((2, T, CW), F32),
            part, part, part, part, part,
            dma((5,)), dma((NH,)), dma((NH,)), dma((NH,)), dma((NW,)), dma((N2,)),
            dma((3,)), dma((3,)),
            dma((NU,)), dma((NU,)), dma((NU,)), dma((NU,)),
            dma((2,)), dma((2,)),
            dma((2,)), dma((NC,)), dma((2,)), dma((NC,)), dma((NC,)), dma((NC,)),
        ],
        compiler_params=pltpu.CompilerParams(
            collective_id=0, has_side_effects=True, vmem_limit_bytes=67000000),
        cost_estimate=pl.CostEstimate(flops=flops, bytes_accessed=6 * E * D * FF, transcendentals=0),
        name='moe',
    )(q, k, v, x, wo.reshape(D, D), ln2.reshape(1, D), meta, w1, w3, w2)


def solution(mesh):
    def local(x, idx, g, hot_tok, hot_g, ln1, wq, wk, wv, wo, ln2, w1, w3, w2):
        n_exp = w1.shape[0] * mesh.shape['expert']
        v, k, q, meta = _qkv(x, ln1, wq, wk, wv, idx, g, hot_tok, hot_g, n_exp)
        return _moe(q, k, v, x, wo, ln2, meta, w1, w3, w2, idx.shape[1])

    tk = ('data', 'expert')
    rep3 = P(None, None, None)
    exp3 = P('expert', None, None)
    return jax.shard_map(
        local, mesh=mesh,
        in_specs=(P(tk, None), P(tk, None), P(tk, None), P(tk), P(tk), P(None),
                  rep3, rep3, rep3, rep3, P(None), exp3, exp3, exp3),
        out_specs=P(tk, None), check_vma=False)
```

```python
import functools

import jax
import jax.numpy as jnp
import numpy as np
from jax import lax
from jax.experimental import pallas as pl
from jax.experimental.pallas import tpu as pltpu
from jax.sharding import PartitionSpec as P

EPS = 1e-6
ROPE_BASE = 10000.0
HOT_ID = 1
SLOTS = 32
F32 = jnp.float32
BF16 = jnp.bfloat16
MESH = pl.DeviceIdType.MESH


def _tables(n_tok, dh):
    half = dh // 2
    freq = np.float32(ROPE_BASE) ** (-np.arange(half, dtype=np.float32) / np.float32(half))
    ang = np.arange(n_tok, dtype=np.float32)[:, None] * freq[None, :].astype(np.float32)
    cos = np.cos(ang).astype(np.float32)
    sin = np.sin(ang).astype(np.float32)
    return np.concatenate([cos, cos], axis=1), np.concatenate([-sin, sin], axis=1)


def _qkv_kernel(n_exp, x_ref, ln1_ref, cos_ref, sin_ref, idx_ref, g_ref, tok_ref, hg_ref, wv, wk, wq,
                v_ref, k_ref, q_ref, meta_ref, wb, acc, ab, sem):
    T, D = x_ref.shape
    _, NB, KB, NH, DH = wb.shape
    ws = (wv, wk, wq)

    def copy(i, b):
        return pltpu.make_async_copy(ws[i].at[pl.ds(b * KB, KB)], wb.at[i, b], sem.at[i, b])

    for i in range(3):
        for b in range(NB):
            copy(i, b).start()

    ss = jnp.zeros((T, 1), F32)
    for c in range(0, D, 512):
        xc = x_ref[:, c:c + 512].astype(F32)
        ss = ss + jnp.sum(xc * xc, axis=1, keepdims=True)
    inv = lax.rsqrt(ss * (1.0 / D) + EPS)
    for c in range(0, D, 512):
        ab[:, c:c + 512] = (x_ref[:, c:c + 512].astype(F32) * inv * ln1_ref[0:1, c:c + 512]).astype(BF16)

    KC = idx_ref.shape[0]
    e_iota = lax.broadcasted_iota(jnp.int32, (n_exp, T), 0)
    hits = [e_iota == idx_ref[j:j + 1, :] for j in range(KC)]
    member = hits[0]
    for h in hits[1:]:
        member = jnp.logical_or(member, h)
    earlier = lax.broadcasted_iota(jnp.int32, (T, T), 0) < lax.broadcasted_iota(jnp.int32, (T, T), 1)
    before = jnp.dot(jnp.where(member, 1.0, 0.0).astype(BF16), jnp.where(earlier, 1.0, 0.0).astype(BF16),
                     preferred_element_type=F32)
    meta_ref[...] = jnp.full((16, T), -1.0, F32)
    for j in range(KC):
        rank = jnp.sum(jnp.where(hits[j], before, 0.0), axis=0, keepdims=True)
        meta_ref[j:j + 1, :] = idx_ref[j:j + 1, :].astype(F32) * SLOTS + rank
        meta_ref[8 + j:9 + j, :] = g_ref[j:j + 1, :]
    tok = jnp.broadcast_to(tok_ref[...].astype(F32), (8, T)).T[:, 0:1]
    hg = jnp.broadcast_to(hg_ref[...], (8, T)).T[:, 0:1]
    t_iota = lax.broadcasted_iota(jnp.int32, (T, T), 1).astype(F32)
    meta_ref[13:14, :] = jnp.sum(jnp.where(tok == t_iota, hg, 0.0), axis=0, keepdims=True)

    for i, out in enumerate((v_ref, k_ref, q_ref)):
        for b in range(NB):
            copy(i, b).wait()
            part = jnp.dot(ab[:, b * KB:(b + 1) * KB], wb[i, b].reshape(KB, D), preferred_element_type=F32)
            if b < NB - 1:
                acc[...] = part if b == 0 else acc[...] + part
                continue
            for h in range(NH):
                t = part[:, h * DH:(h + 1) * DH]
                if NB > 1:
                    t = t + acc[:, h * DH:(h + 1) * DH]
                if i > 0:
                    t = t * cos_ref[...] + pltpu.roll(t, DH // 2, 1) * sin_ref[...]
                out[:, h * DH:(h + 1) * DH] = t.astype(BF16)


def _qkv(x, ln1, wq, wk, wv, idx, g, hot_tok, hot_g, n_exp):
    T, D = x.shape
    _, NH, DH = wq.shape
    NB = 2
    cos, sin = _tables(T, DH)
    vm = pl.BlockSpec(memory_space=pltpu.VMEM)
    any_spec = pl.BlockSpec(memory_space=pl.ANY)
    head = jax.ShapeDtypeStruct((T, D), BF16)
    return pl.pallas_call(
        functools.partial(_qkv_kernel, n_exp),
        out_shape=[head, head, head, jax.ShapeDtypeStruct((16, T), F32)],
        in_specs=[vm] * 8 + [any_spec] * 3,
        out_specs=[vm] * 4,
        scratch_shapes=[
            pltpu.VMEM((3, NB, D // NB, NH, DH), BF16),
            pltpu.VMEM((T, D), F32),
            pltpu.VMEM((T, D), BF16),
            pltpu.SemaphoreType.DMA((3, NB)),
        ],
        compiler_params=pltpu.CompilerParams(vmem_limit_bytes=60000000),
        cost_estimate=pl.CostEstimate(flops=6 * T * D * D, bytes_accessed=6 * D * D, transcendentals=0),
        name='qkv',
    )(x, ln1.reshape(1, D), jnp.asarray(cos), jnp.asarray(sin), idx.T, g.T, hot_tok.reshape(1, T),
      hot_g.reshape(1, T), wv, wk, wq)


NU = 4
NW = 5
G2 = 8


def _moe_kernel(KC, CW, DH, q_hbm, k_hbm, v_hbm, x_hbm, wo, ln2_ref, meta_hbm, w1, w3, w2, y_ref,
                u_all, meta, xs, zt, zh, wbuf, ob, cm, sel, hgc, zhot, sdiag, ssib, scpt, own, rdiag, rsib, rcpt,
                in_sem, qkv_sem, wsem, w2sem, um_send, um_recv, uc_send, uc_recv, uf_send, uf_recv,
                us_send, us_recv, dg_send, dg_recv, sb_send, sb_recv, cp_send, cp_recv):
    me = lax.axis_index('expert')
    core = me % 2
    sib = me + 1 - 2 * core
    cpt = (me + 2) % 4
    E, D, FF = w1.shape
    T = q_hbm.shape[0]
    NH = D // DH
    HT = T // 2
    QW = 512
    PB = 4
    R = E * SLOTS
    NC = D // CW
    RU = T // NU

    def start_w(i, src, odd):
        e = (i + HOT_ID) % E
        b = (2 * i + odd) % NW
        pltpu.make_async_copy(src.at[e], wbuf.at[b], wsem.at[b]).start()

    def wait_w(i, src, odd):
        b = (2 * i + odd) % NW
        pltpu.make_async_copy(src.at[0], wbuf.at[b], wsem.at[b]).wait()

    N2 = NW * PB
    B2 = (2 * E) % NW

    def w2_slot(t):
        sl = t % N2
        return (B2 + sl // PB) % NW, pl.ds(0, FF), pl.ds(pl.multiple_of((sl % PB) * CW, CW), CW)

    def w2_dst(t):
        return wbuf.at[w2_slot(t)], w2sem.at[t % N2]

    def start_w2(t):
        dst, sem = w2_dst(t)
        e = (t % E + HOT_ID) % E
        c = t // E
        pltpu.make_async_copy(w2.at[e, :, pl.ds(pl.multiple_of(c * CW, CW), CW)], dst, sem).start()

    def wait_w2(t):
        dst, sem = w2_dst(t)
        pltpu.make_async_copy(w2.at[0, :, pl.ds(0, CW)], dst, sem).wait()

    HB = QW // DH
    QB, KB, VB = 4, 6, 8
    qkv = [[pltpu.make_async_copy(src.at[pl.ds(i * HT, HT)], xs.at[b + i], qkv_sem.at[n, i])
            for n, (src, b) in enumerate(((q_hbm, QB), (k_hbm, KB), (v_hbm, VB)))] for i in range(2)]
    for c in qkv[0] + qkv[1]:
        c.start()
    cx = [pltpu.make_async_copy(x_hbm.at[pl.ds(i * HT, HT)], xs.at[2 + i], in_sem.at[i]) for i in range(2)]
    cwo = [pltpu.make_async_copy(wo.at[:, pl.ds(i * D // 2, D // 2)], wbuf.at[2 + i, :, pl.ds(0, D // 2)],
                                 in_sem.at[2 + i]) for i in range(2)]
    cm_ = pltpu.make_async_copy(meta_hbm, meta.at[0], in_sem.at[4])
    for c in cx + cwo + [cm_]:
        c.start()
    start_w(0, w1, 0)
    start_w(0, w3, 1)
    start_w(2, w1, 0)

    barrier = pltpu.get_barrier_semaphore()
    for peer in (sib, cpt):
        pl.semaphore_signal(barrier, inc=1, device_id={'expert': peer}, device_id_type=MESH)

    def remote(src, dst, ss, rs, peer):
        return pltpu.make_async_remote_copy(src_ref=src, dst_ref=dst, send_sem=ss, recv_sem=rs,
                                            device_id={'expert': peer}, device_id_type=MESH)

    m_sib = remote(meta.at[0], meta.at[1], um_send.at[0], um_recv.at[0], sib)
    m_cpt = remote(meta.at[0], meta.at[2], um_send.at[1], um_recv.at[1], cpt)
    m_fwd = remote(meta.at[2], meta.at[3], um_send.at[2], um_recv.at[2], sib)
    u_sib = [remote(u_all.at[0, pl.ds(i * HT, HT)], u_all.at[1, pl.ds(i * HT, HT)], us_send.at[i], us_recv.at[i], sib)
             for i in range(2)]

    def u_cpt(k):
        r = pl.ds(k * RU, RU)
        return remote(u_all.at[0, r], u_all.at[2, r], uc_send.at[k], uc_recv.at[k], cpt)

    def u_fwd(k):
        r = pl.ds(k * RU, RU)
        return remote(u_all.at[2, r], u_all.at[3, r], uf_send.at[k], uf_recv.at[k], sib)

    scale = DH ** -0.5

    def attend(half):
        r0 = half * HT
        nk = r0 + HT
        row = lax.broadcasted_iota(jnp.int32, (HT, nk), 0) + r0
        seen = row >= lax.broadcasted_iota(jnp.int32, (HT, nk), 1)

        for c in qkv[half]:
            c.wait()

        def heads(c, carry):
            lanes = [pl.ds(pl.multiple_of(c * QW + j * DH, DH), DH) for j in range(HB)]

            def rows(b, ls):
                return jnp.concatenate([xs[b + i, :, ls] for i in range(half + 1)], axis=0)

            sc = [lax.dot_general(xs[QB + half, :, ls], rows(KB, ls), (((1,), (1,)), ((), ())),
                                  preferred_element_type=F32) for ls in lanes]
            sc = [jnp.where(seen, s * scale, -jnp.inf) for s in sc]
            ps = [jnp.exp(s - jnp.max(s, axis=1, keepdims=True)) for s in sc]
            ps = [(p * (1.0 / jnp.sum(p, axis=1, keepdims=True))).astype(BF16) for p in ps]
            os = [jnp.dot(p, rows(VB, ls), preferred_element_type=F32) for p, ls in zip(ps, lanes)]
            for o, ls in zip(os, lanes):
                xs[half, :, ls] = o.astype(BF16)
            return carry

        lax.fori_loop(0, NH // HB, heads, 0)
        cx[half].wait()
        if half == 0:
            cwo[0].wait()
            cwo[1].wait()
        ss = jnp.zeros((HT, 1), F32)
        for n in range(D // QW):
            wn = (n * QW) // (D // 2)
            w0 = n * QW - wn * (D // 2)
            o = jnp.dot(xs[half], wbuf[2 + wn, :, w0:w0 + QW], preferred_element_type=F32)
            for z in range(QW // CW):
                c0 = n * QW + z * CW
                h = (xs[2 + half, :, c0:c0 + CW].astype(F32) + o[:, z * CW:(z + 1) * CW]).astype(BF16).astype(F32)
                own[c0 // CW, 0:HT, :] = h
                ss = ss + jnp.sum(h * h, axis=1, keepdims=True)
        inv = lax.rsqrt(ss * (1.0 / D) + EPS)
        for n in range(NC):
            cs = slice(n * CW, (n + 1) * CW)
            u_all[0, r0:nk, cs] = (own[n, 0:HT, :] * inv * ln2_ref[0:1, cs]).astype(BF16)

    attend(0)
    cm_.wait()
    pl.semaphore_wait(barrier, 2)
    m_cpt.start()
    for k in range(NU // 2):
        u_cpt(k).start()
    m_sib.start()
    u_sib[0].start()
    attend(1)
    for k in range(NU // 2, NU):
        u_cpt(k).start()
    u_sib[1].start()
    start_w(1, w1, 0)
    start_w(1, w3, 1)

    base = (me * R).astype(F32)

    def select(s):
        mt = meta[s]
        slot_iota = lax.broadcasted_iota(jnp.int32, (R, T), 0).astype(F32)
        hit = slot_iota == (mt[0:1, :] - base)
        for j in range(1, KC):
            hit = jnp.logical_or(hit, slot_iota == (mt[j:j + 1, :] - base))
        sel[s] = jnp.where(hit, 1.0, 0.0).astype(BF16)
        mc = mt.T
        lane = lax.broadcasted_iota(jnp.int32, (T, R), 1).astype(F32)
        gate = jnp.zeros((T, R), F32)
        for j in range(KC):
            gate = gate + jnp.where(lane == (mc[:, j:j + 1] - base), mc[:, 8 + j:9 + j], 0.0)
        hi = gate.astype(BF16)
        r1 = gate - hi.astype(F32)
        mid = r1.astype(BF16)
        lo = (r1 - mid.astype(F32)).astype(BF16)
        hgc[s] = mc[:, 13:14]
        cm[s, 0:T, :] = hi
        cm[s, T:2 * T, :] = mid
        cm[s, 2 * T:3 * T, :] = lo

    def dispatch(s):
        for c in range(D // 512):
            cs = slice(c * 512, c * 512 + 512)
            part = jnp.dot(sel[s], u_all[s, :, cs], preferred_element_type=F32).astype(BF16)
            xs[:, s * SLOTS:(s + 1) * SLOTS, cs] = part.reshape(E, SLOTS, 512)

    cols = [(0, 512), (512, 512), (1024, FF - 1024)]

    def hot_local(s, carry):
        for c0, cn in cols:
            a = u_all[s]
            h1 = jnp.dot(a, wbuf[0, :, c0:c0 + cn], preferred_element_type=F32)
            h3 = jnp.dot(a, wbuf[1, :, c0:c0 + cn], preferred_element_type=F32)
            zh[s, :, c0:c0 + cn] = (jax.nn.silu(h1) * h3).astype(BF16)
        return carry

    def hot_batch(k):
        r = pl.ds(pl.multiple_of(k * RU, RU), RU)
        a = jnp.concatenate([u_all[2, r, :], u_all[3, r, :]], axis=0)
        for c0, cn in cols:
            h1 = jnp.dot(a, wbuf[0, :, c0:c0 + cn], preferred_element_type=F32)
            h3 = jnp.dot(a, wbuf[1, :, c0:c0 + cn], preferred_element_type=F32)
            z = (jax.nn.silu(h1) * h3).astype(BF16)
            zh[2, r, c0:c0 + cn] = z[0:RU]
            zh[3, r, c0:c0 + cn] = z[RU:]

    def cold_up(e, b):
        for c0, cn in cols:
            a = xs[e]
            h1 = jnp.dot(a, wbuf[b, :, c0:c0 + cn], preferred_element_type=F32)
            h3 = jnp.dot(a, wbuf[(b + 1) % NW, :, c0:c0 + cn], preferred_element_type=F32)
            zt[:, c0:c0 + cn] = (jax.nn.silu(h1) * h3).astype(BF16)
        xs[e, :, 0:FF] = zt[...]

    select(0)
    dispatch(0)
    m_sib.wait_recv()
    select(1)
    m_cpt.wait_recv()
    m_fwd.start()
    select(2)
    for i in range(2):
        u_sib[i].wait_recv()
    dispatch(1)
    wait_w(0, w1, 0)
    wait_w(0, w3, 1)

    @pl.when(me == 0)
    def _():
        lax.fori_loop(0, 2, hot_local, 0)

    m_fwd.wait_recv()
    select(3)
    u_cpt(0).wait_recv()
    u_fwd(0).start()

    def arrive(k, carry):
        u_fwd(k - 1).wait_recv()

        @pl.when(me == 0)
        def _():
            hot_batch(k - 1)

        u_cpt(k).wait_recv()
        u_fwd(k).start()
        return carry

    lax.fori_loop(1, NU, arrive, 0)
    dispatch(2)
    u_fwd(NU - 1).wait_recv()
    dispatch(3)

    @pl.when(me == 0)
    def _():
        hot_batch(NU - 1)

    @pl.when(me != 0)
    def _():
        cold_up(HOT_ID, 0)

    start_w(2, w3, 1)
    start_w(3, w1, 0)

    def up_step(i, carry):
        e = (i + HOT_ID) % E
        b = (2 * i) % NW
        wait_w(i, w1, 0)
        wait_w(i, w3, 1)
        cold_up(e, b)

        @pl.when(i < E - 2)
        def _():
            start_w(i + 2, w3, 1)

        @pl.when(i < E - 3)
        def _():
            start_w(i + 3, w1, 0)

        @pl.when(i >= E - 3)
        def _():
            n0 = (i - (E - 3)) * 2 * PB
            for q in range(PB):
                start_w2(n0 - PB + q + PB * ((E - 1 - i) // 2))

        @pl.when(i >= E - 2)
        def _():
            n0 = (i - (E - 3)) * 2 * PB
            for q in range(PB):
                start_w2(n0 + q)
        return carry

    lax.fori_loop(1, E, up_step, 0)

    def chunk(c, carry):
        def cold_down(t):
            e = (t % E + HOT_ID) % E
            o = jnp.dot(xs[e, :, 0:FF], wbuf[w2_slot(t)], preferred_element_type=F32).astype(BF16)
            ob[:, pl.ds(pl.multiple_of(e * SLOTS, SLOTS), SLOTS), :] = o.reshape(4, SLOTS, CW)

        wait_w2(c * E)

        @pl.when(me == 0)
        def _():
            def hot_down(s, carry2):
                z = zh[pl.ds(2 * s, 2)].reshape(2 * T, FF)
                o = jnp.dot(z, wbuf[w2_slot(c * E)], preferred_element_type=F32).astype(BF16)
                for q in range(2):
                    zhot[2 * s + q] = hgc[2 * s + q] * o[q * T:(q + 1) * T].astype(F32)
                return carry2

            lax.fori_loop(0, 2, hot_down, 0)

        def down(i, carry2):
            t0 = c * E + i * G2

            @pl.when(i > 0)
            def _():
                wait_w2(t0)

            for q in range(1, G2):
                wait_w2(t0 + q)
            for q in range(G2):
                cold_down(t0 + q)
            for p in range(0, G2, PB):
                @pl.when(t0 + N2 + p < NC * E)
                def _():
                    for q in range(PB):
                        start_w2(t0 + N2 + p + q)
            return carry2

        lax.fori_loop(0, E // G2, down, 0)

        def combine(s):
            r = jnp.dot(cm[s], ob[s], preferred_element_type=F32)
            return (r[0:T] + r[T:2 * T]) + r[2 * T:3 * T] + zhot[s]

        p = c % 2
        d_cp = remote(sdiag.at[p], rdiag.at[c], dg_send.at[p], dg_recv.at[c], sib)
        s_cp = remote(ssib.at[p], rsib.at[c], sb_send.at[p], sb_recv.at[c], sib)
        x_cp = remote(scpt.at[c], rcpt.at[c], cp_send.at[c], cp_recv.at[c], cpt)

        @pl.when(c >= 2)
        def _():
            d_cp.wait_send()
            s_cp.wait_send()

        sdiag[p] = combine(3)
        d_cp.start()
        ssib[p] = combine(1)
        s_cp.start()
        scpt[c] = combine(2)
        own[c] = combine(0)
        d_cp.wait_recv()
        scpt[c] = scpt[c] + rdiag[c]
        x_cp.start()
        return carry

    zhot[...] = jnp.zeros_like(zhot)
    lax.fori_loop(0, NC, chunk, 0)

    for c in range(NC):
        cs = slice(c * CW, c * CW + CW)
        remote(ssib.at[0], rsib.at[c], sb_send.at[0], sb_recv.at[c], sib).wait_recv()
        remote(scpt.at[c], rcpt.at[c], cp_send.at[c], cp_recv.at[c], cpt).wait_recv()
        y_ref[:, cs] = (own[c] + rsib[c] + rcpt[c]).astype(BF16)

    m_sib.wait_send()
    m_cpt.wait_send()
    m_fwd.wait_send()
    for i in range(2):
        u_sib[i].wait_send()
    for k in range(NU):
        u_cpt(k).wait_send()
        u_fwd(k).wait_send()
    for p in range(2):
        remote(sdiag.at[p], rdiag.at[p], dg_send.at[p], dg_recv.at[p], sib).wait_send()
        remote(ssib.at[p], rsib.at[p], sb_send.at[p], sb_recv.at[p], sib).wait_send()
    for c in range(NC):
        remote(scpt.at[c], rcpt.at[c], cp_send.at[c], cp_recv.at[c], cpt).wait_send()


def _moe(q, k, v, x, wo, ln2, meta, w1, w3, w2, KC, DH):
    T, D = x.shape
    E, _, FF = w1.shape
    CW = 256
    NC = D // CW
    R = E * SLOTS
    dma = pltpu.SemaphoreType.DMA
    vm = pl.BlockSpec(memory_space=pltpu.VMEM)
    any_spec = pl.BlockSpec(memory_space=pl.ANY)
    part = pltpu.VMEM((NC, T, CW), F32)
    flops = 6 * D * FF * (E * 4 * SLOTS + T)
    return pl.pallas_call(
        functools.partial(_moe_kernel, KC, CW, DH),
        out_shape=jax.ShapeDtypeStruct((T, D), BF16),
        in_specs=[any_spec] * 5 + [vm] + [any_spec] * 4,
        out_specs=pl.BlockSpec(memory_space=pltpu.VMEM),
        scratch_shapes=[
            pltpu.VMEM((4, T, D), BF16),
            pltpu.VMEM((4, 16, T), F32),
            pltpu.VMEM((E, 4 * SLOTS, D), BF16),
            pltpu.VMEM((4 * SLOTS, FF), BF16),
            pltpu.VMEM((4, T, FF), BF16),
            pltpu.VMEM((NW, D, FF), BF16),
            pltpu.VMEM((4, R, CW), BF16),
            pltpu.VMEM((4, 3 * T, R), BF16),
            pltpu.VMEM((4, R, T), BF16),
            pltpu.VMEM((4, T, 1), F32),
            pltpu.VMEM((4, T, CW), F32),
            pltpu.VMEM((2, T, CW), F32),
            pltpu.VMEM((2, T, CW), F32),
            part, part, part, part, part,
            dma((5,)), dma((3, 2)), dma((NW,)), dma((NW * 4,)),
            dma((3,)), dma((3,)),
            dma((NU,)), dma((NU,)), dma((NU,)), dma((NU,)),
            dma((2,)), dma((2,)),
            dma((2,)), dma((NC,)), dma((2,)), dma((NC,)), dma((NC,)), dma((NC,)),
        ],
        compiler_params=pltpu.CompilerParams(
            collective_id=0, has_side_effects=True, vmem_limit_bytes=67000000),
        cost_estimate=pl.CostEstimate(flops=flops, bytes_accessed=6 * E * D * FF, transcendentals=0),
        name='moe',
    )(q, k, v, x, wo.reshape(D, D), ln2.reshape(1, D), meta, w1, w3, w2)


def solution(mesh):
    def local(x, idx, g, hot_tok, hot_g, ln1, wq, wk, wv, wo, ln2, w1, w3, w2):
        n_exp = w1.shape[0] * mesh.shape['expert']
        v, k, q, meta = _qkv(x, ln1, wq, wk, wv, idx, g, hot_tok, hot_g, n_exp)
        return _moe(q, k, v, x, wo, ln2, meta, w1, w3, w2, idx.shape[1], wq.shape[2])

    tk = ('data', 'expert')
    rep3 = P(None, None, None)
    exp3 = P('expert', None, None)
    return jax.shard_map(
        local, mesh=mesh,
        in_specs=(P(tk, None), P(tk, None), P(tk, None), P(tk), P(tk), P(None),
                  rep3, rep3, rep3, rep3, P(None), exp3, exp3, exp3),
        out_specs=P(tk, None), check_vma=False)
```

```python
import functools

import jax
import jax.numpy as jnp
import numpy as np
from jax import lax
from jax.experimental import pallas as pl
from jax.experimental.pallas import tpu as pltpu
from jax.sharding import PartitionSpec as P

EPS = 1e-6
ROPE_BASE = 10000.0
HOT_ID = 1
SLOTS = 32
F32 = jnp.float32
BF16 = jnp.bfloat16
MESH = pl.DeviceIdType.MESH


def _tables(n_tok, dh):
    half = dh // 2
    freq = np.float32(ROPE_BASE) ** (-np.arange(half, dtype=np.float32) / np.float32(half))
    ang = np.arange(n_tok, dtype=np.float32)[:, None] * freq[None, :].astype(np.float32)
    cos = np.cos(ang).astype(np.float32)
    sin = np.sin(ang).astype(np.float32)
    return np.concatenate([cos, cos], axis=1), np.concatenate([-sin, sin], axis=1)


def _qkv_kernel(n_exp, x_ref, ln1_ref, cos_ref, sin_ref, idx_ref, g_ref, tok_ref, hg_ref, wv, wk, wq,
                v_ref, k_ref, q_ref, meta_ref, wb, acc, ab, sem):
    T, D = x_ref.shape
    _, NB, KB, NH, DH = wb.shape
    ws = (wv, wk, wq)

    def copy(i, b):
        return pltpu.make_async_copy(ws[i].at[pl.ds(b * KB, KB)], wb.at[i, b], sem.at[i, b])

    for i in range(3):
        for b in range(NB):
            copy(i, b).start()

    ss = jnp.zeros((T, 1), F32)
    for c in range(0, D, 512):
        xc = x_ref[:, c:c + 512].astype(F32)
        ss = ss + jnp.sum(xc * xc, axis=1, keepdims=True)
    inv = lax.rsqrt(ss * (1.0 / D) + EPS)
    for c in range(0, D, 512):
        ab[:, c:c + 512] = (x_ref[:, c:c + 512].astype(F32) * inv * ln1_ref[0:1, c:c + 512]).astype(BF16)

    KC = idx_ref.shape[0]
    e_iota = lax.broadcasted_iota(jnp.int32, (n_exp, T), 0)
    hits = [e_iota == idx_ref[j:j + 1, :] for j in range(KC)]
    member = hits[0]
    for h in hits[1:]:
        member = jnp.logical_or(member, h)
    earlier = lax.broadcasted_iota(jnp.int32, (T, T), 0) < lax.broadcasted_iota(jnp.int32, (T, T), 1)
    before = jnp.dot(jnp.where(member, 1.0, 0.0).astype(BF16), jnp.where(earlier, 1.0, 0.0).astype(BF16),
                     preferred_element_type=F32)
    meta_ref[...] = jnp.full((16, T), -1.0, F32)
    for j in range(KC):
        rank = jnp.sum(jnp.where(hits[j], before, 0.0), axis=0, keepdims=True)
        meta_ref[j:j + 1, :] = idx_ref[j:j + 1, :].astype(F32) * SLOTS + rank
        meta_ref[8 + j:9 + j, :] = g_ref[j:j + 1, :]
    tok = jnp.broadcast_to(tok_ref[...].astype(F32), (8, T)).T[:, 0:1]
    hg = jnp.broadcast_to(hg_ref[...], (8, T)).T[:, 0:1]
    t_iota = lax.broadcasted_iota(jnp.int32, (T, T), 1).astype(F32)
    meta_ref[13:14, :] = jnp.sum(jnp.where(tok == t_iota, hg, 0.0), axis=0, keepdims=True)

    for i, out in enumerate((v_ref, k_ref, q_ref)):
        for b in range(NB):
            copy(i, b).wait()
            part = jnp.dot(ab[:, b * KB:(b + 1) * KB], wb[i, b].reshape(KB, D), preferred_element_type=F32)
            if b < NB - 1:
                acc[...] = part if b == 0 else acc[...] + part
                continue
            for h in range(NH):
                t = part[:, h * DH:(h + 1) * DH]
                if NB > 1:
                    t = t + acc[:, h * DH:(h + 1) * DH]
                if i > 0:
                    t = t * cos_ref[...] + pltpu.roll(t, DH // 2, 1) * sin_ref[...]
                out[:, h * DH:(h + 1) * DH] = t.astype(BF16)


def _qkv(x, ln1, wq, wk, wv, idx, g, hot_tok, hot_g, n_exp):
    T, D = x.shape
    _, NH, DH = wq.shape
    NB = 2
    cos, sin = _tables(T, DH)
    vm = pl.BlockSpec(memory_space=pltpu.VMEM)
    any_spec = pl.BlockSpec(memory_space=pl.ANY)
    head = jax.ShapeDtypeStruct((T, D), BF16)
    return pl.pallas_call(
        functools.partial(_qkv_kernel, n_exp),
        out_shape=[head, head, head, jax.ShapeDtypeStruct((16, T), F32)],
        in_specs=[vm] * 8 + [any_spec] * 3,
        out_specs=[vm] * 4,
        scratch_shapes=[
            pltpu.VMEM((3, NB, D // NB, NH, DH), BF16),
            pltpu.VMEM((T, D), F32),
            pltpu.VMEM((T, D), BF16),
            pltpu.SemaphoreType.DMA((3, NB)),
        ],
        compiler_params=pltpu.CompilerParams(vmem_limit_bytes=60000000),
        cost_estimate=pl.CostEstimate(flops=6 * T * D * D, bytes_accessed=6 * D * D, transcendentals=0),
        name='qkv',
    )(x, ln1.reshape(1, D), jnp.asarray(cos), jnp.asarray(sin), idx.T, g.T, hot_tok.reshape(1, T),
      hot_g.reshape(1, T), wv, wk, wq)


NU = 4
NW = 5
G2 = 8


def _moe_kernel(KC, CW, DH, q_hbm, k_hbm, v_hbm, x_hbm, wo, ln2_ref, meta_hbm, w1, w3, w2, y_ref,
                u_all, meta, xs, zt, zh, wbuf, ob, cm, sel, hgc, zhot, sdiag, ssib, scpt, own, rdiag, rsib, rcpt,
                in_sem, qkv_sem, wsem, w2sem, um_send, um_recv, uc_send, uc_recv, uf_send, uf_recv,
                us_send, us_recv, dg_send, dg_recv, sb_send, sb_recv, cp_send, cp_recv):
    me = lax.axis_index('expert')
    core = me % 2
    sib = me + 1 - 2 * core
    cpt = (me + 2) % 4
    E, D, FF = w1.shape
    T = q_hbm.shape[0]
    NH = D // DH
    HT = T // 2
    QW = 512
    PB = 4
    R = E * SLOTS
    NC = D // CW
    RU = T // NU

    def start_w(i, src, odd):
        e = (i + HOT_ID) % E
        b = (2 * i + odd) % NW
        pltpu.make_async_copy(src.at[e], wbuf.at[b], wsem.at[b]).start()

    def wait_w(i, src, odd):
        b = (2 * i + odd) % NW
        pltpu.make_async_copy(src.at[0], wbuf.at[b], wsem.at[b]).wait()

    N2 = NW * PB
    B2 = (2 * E) % NW

    def w2_slot(t):
        sl = t % N2
        return (B2 + sl // PB) % NW, pl.ds(0, FF), pl.ds(pl.multiple_of((sl % PB) * CW, CW), CW)

    def w2_dst(t):
        return wbuf.at[w2_slot(t)], w2sem.at[t % N2]

    def start_w2(t):
        dst, sem = w2_dst(t)
        e = (t % E + HOT_ID) % E
        c = t // E
        pltpu.make_async_copy(w2.at[e, :, pl.ds(pl.multiple_of(c * CW, CW), CW)], dst, sem).start()

    def wait_w2(t):
        dst, sem = w2_dst(t)
        pltpu.make_async_copy(w2.at[0, :, pl.ds(0, CW)], dst, sem).wait()

    HB = QW // DH
    QB, KB, VB = 4, 6, 8
    qkv = [[pltpu.make_async_copy(src.at[pl.ds(i * HT, HT)], xs.at[b + i], qkv_sem.at[n, i])
            for n, (src, b) in enumerate(((q_hbm, QB), (k_hbm, KB), (v_hbm, VB)))] for i in range(2)]
    for c in qkv[0] + qkv[1]:
        c.start()
    cx = [pltpu.make_async_copy(x_hbm.at[pl.ds(i * HT, HT)], xs.at[2 + i], in_sem.at[i]) for i in range(2)]
    cwo = [pltpu.make_async_copy(wo.at[:, pl.ds(i * D // 2, D // 2)], wbuf.at[2 + i, :, pl.ds(0, D // 2)],
                                 in_sem.at[2 + i]) for i in range(2)]
    cm_ = pltpu.make_async_copy(meta_hbm, meta.at[0], in_sem.at[4])
    for c in cx + cwo + [cm_]:
        c.start()
    barrier = pltpu.get_barrier_semaphore()
    for peer in (sib, cpt):
        pl.semaphore_signal(barrier, inc=1, device_id={'expert': peer}, device_id_type=MESH)

    def remote(src, dst, ss, rs, peer):
        return pltpu.make_async_remote_copy(src_ref=src, dst_ref=dst, send_sem=ss, recv_sem=rs,
                                            device_id={'expert': peer}, device_id_type=MESH)

    m_sib = remote(meta.at[0], meta.at[1], um_send.at[0], um_recv.at[0], sib)
    m_cpt = remote(meta.at[0], meta.at[2], um_send.at[1], um_recv.at[1], cpt)
    m_fwd = remote(meta.at[2], meta.at[3], um_send.at[2], um_recv.at[2], sib)
    u_sib = [remote(u_all.at[0, pl.ds(i * HT, HT)], u_all.at[1, pl.ds(i * HT, HT)], us_send.at[i], us_recv.at[i], sib)
             for i in range(2)]

    def u_cpt(k):
        r = pl.ds(k * RU, RU)
        return remote(u_all.at[0, r], u_all.at[2, r], uc_send.at[k], uc_recv.at[k], cpt)

    def u_fwd(k):
        r = pl.ds(k * RU, RU)
        return remote(u_all.at[2, r], u_all.at[3, r], uf_send.at[k], uf_recv.at[k], sib)

    scale = DH ** -0.5

    def attend(half):
        r0 = half * HT
        nk = r0 + HT
        row = lax.broadcasted_iota(jnp.int32, (HT, nk), 0) + r0
        seen = row >= lax.broadcasted_iota(jnp.int32, (HT, nk), 1)

        for c in qkv[half]:
            c.wait()

        def heads(c, carry):
            lanes = [pl.ds(pl.multiple_of(c * QW + j * DH, DH), DH) for j in range(HB)]

            def rows(b, ls):
                return jnp.concatenate([xs[b + i, :, ls] for i in range(half + 1)], axis=0)

            sc = [lax.dot_general(xs[QB + half, :, ls], rows(KB, ls), (((1,), (1,)), ((), ())),
                                  preferred_element_type=F32) for ls in lanes]
            sc = [jnp.where(seen, s * scale, -jnp.inf) for s in sc]
            ps = [jnp.exp(s - jnp.max(s, axis=1, keepdims=True)) for s in sc]
            ps = [(p * (1.0 / jnp.sum(p, axis=1, keepdims=True))).astype(BF16) for p in ps]
            os = [jnp.dot(p, rows(VB, ls), preferred_element_type=F32) for p, ls in zip(ps, lanes)]
            for o, ls in zip(os, lanes):
                xs[half, :, ls] = o.astype(BF16)
            return carry

        lax.fori_loop(0, NH // HB, heads, 0)
        cx[half].wait()
        if half == 0:
            cwo[0].wait()
            cwo[1].wait()
            start_w(0, w1, 0)
            start_w(0, w3, 1)
            start_w(2, w1, 0)
        ss = jnp.zeros((HT, 1), F32)
        for n in range(D // QW):
            wn = (n * QW) // (D // 2)
            w0 = n * QW - wn * (D // 2)
            o = jnp.dot(xs[half], wbuf[2 + wn, :, w0:w0 + QW], preferred_element_type=F32)
            for z in range(QW // CW):
                c0 = n * QW + z * CW
                h = (xs[2 + half, :, c0:c0 + CW].astype(F32) + o[:, z * CW:(z + 1) * CW]).astype(BF16).astype(F32)
                own[c0 // CW, 0:HT, :] = h
                ss = ss + jnp.sum(h * h, axis=1, keepdims=True)
        inv = lax.rsqrt(ss * (1.0 / D) + EPS)
        for n in range(NC):
            cs = slice(n * CW, (n + 1) * CW)
            u_all[0, r0:nk, cs] = (own[n, 0:HT, :] * inv * ln2_ref[0:1, cs]).astype(BF16)

    attend(0)
    cm_.wait()
    pl.semaphore_wait(barrier, 2)
    m_cpt.start()
    for k in range(NU // 2):
        u_cpt(k).start()
    m_sib.start()
    u_sib[0].start()
    attend(1)
    for k in range(NU // 2, NU):
        u_cpt(k).start()
    u_sib[1].start()
    start_w(1, w1, 0)
    start_w(1, w3, 1)

    base = (me * R).astype(F32)

    def select(s):
        mt = meta[s]
        slot_iota = lax.broadcasted_iota(jnp.int32, (R, T), 0).astype(F32)
        hit = slot_iota == (mt[0:1, :] - base)
        for j in range(1, KC):
            hit = jnp.logical_or(hit, slot_iota == (mt[j:j + 1, :] - base))
        sel[s] = jnp.where(hit, 1.0, 0.0).astype(BF16)
        mc = mt.T
        lane = lax.broadcasted_iota(jnp.int32, (T, R), 1).astype(F32)
        gate = jnp.zeros((T, R), F32)
        for j in range(KC):
            gate = gate + jnp.where(lane == (mc[:, j:j + 1] - base), mc[:, 8 + j:9 + j], 0.0)
        hi = gate.astype(BF16)
        r1 = gate - hi.astype(F32)
        mid = r1.astype(BF16)
        lo = (r1 - mid.astype(F32)).astype(BF16)
        hgc[s] = mc[:, 13:14]
        cm[s, 0:T, :] = hi
        cm[s, T:2 * T, :] = mid
        cm[s, 2 * T:3 * T, :] = lo

    def dispatch(s):
        for c in range(D // 512):
            cs = slice(c * 512, c * 512 + 512)
            part = jnp.dot(sel[s], u_all[s, :, cs], preferred_element_type=F32).astype(BF16)
            xs[:, s * SLOTS:(s + 1) * SLOTS, cs] = part.reshape(E, SLOTS, 512)

    cols = [(0, 512), (512, 512), (1024, FF - 1024)]

    def hot_local(s, carry):
        for c0, cn in cols:
            a = u_all[s]
            h1 = jnp.dot(a, wbuf[0, :, c0:c0 + cn], preferred_element_type=F32)
            h3 = jnp.dot(a, wbuf[1, :, c0:c0 + cn], preferred_element_type=F32)
            zh[s, :, c0:c0 + cn] = (jax.nn.silu(h1) * h3).astype(BF16)
        return carry

    def hot_batch(k):
        r = pl.ds(pl.multiple_of(k * RU, RU), RU)
        a = jnp.concatenate([u_all[2, r, :], u_all[3, r, :]], axis=0)
        for c0, cn in cols:
            h1 = jnp.dot(a, wbuf[0, :, c0:c0 + cn], preferred_element_type=F32)
            h3 = jnp.dot(a, wbuf[1, :, c0:c0 + cn], preferred_element_type=F32)
            z = (jax.nn.silu(h1) * h3).astype(BF16)
            zh[2, r, c0:c0 + cn] = z[0:RU]
            zh[3, r, c0:c0 + cn] = z[RU:]

    def cold_up(e, b):
        for c0, cn in cols:
            a = xs[e]
            h1 = jnp.dot(a, wbuf[b, :, c0:c0 + cn], preferred_element_type=F32)
            h3 = jnp.dot(a, wbuf[(b + 1) % NW, :, c0:c0 + cn], preferred_element_type=F32)
            zt[:, c0:c0 + cn] = (jax.nn.silu(h1) * h3).astype(BF16)
        xs[e, :, 0:FF] = zt[...]

    select(0)
    dispatch(0)
    m_sib.wait_recv()
    select(1)
    m_cpt.wait_recv()
    m_fwd.start()
    select(2)
    for i in range(2):
        u_sib[i].wait_recv()
    dispatch(1)
    wait_w(0, w1, 0)
    wait_w(0, w3, 1)

    @pl.when(me == 0)
    def _():
        lax.fori_loop(0, 2, hot_local, 0)

    m_fwd.wait_recv()
    select(3)
    u_cpt(0).wait_recv()
    u_fwd(0).start()

    def arrive(k, carry):
        u_fwd(k - 1).wait_recv()

        @pl.when(me == 0)
        def _():
            hot_batch(k - 1)

        u_cpt(k).wait_recv()
        u_fwd(k).start()
        return carry

    lax.fori_loop(1, NU, arrive, 0)
    dispatch(2)
    u_fwd(NU - 1).wait_recv()
    dispatch(3)

    @pl.when(me == 0)
    def _():
        hot_batch(NU - 1)

    @pl.when(me != 0)
    def _():
        cold_up(HOT_ID, 0)

    start_w(2, w3, 1)
    start_w(3, w1, 0)

    def up_step(i, carry):
        e = (i + HOT_ID) % E
        b = (2 * i) % NW
        wait_w(i, w1, 0)
        wait_w(i, w3, 1)
        cold_up(e, b)

        @pl.when(i < E - 2)
        def _():
            start_w(i + 2, w3, 1)

        @pl.when(i < E - 3)
        def _():
            start_w(i + 3, w1, 0)

        @pl.when(i >= E - 3)
        def _():
            n0 = (i - (E - 3)) * 2 * PB
            for q in range(PB):
                start_w2(n0 - PB + q + PB * ((E - 1 - i) // 2))

        @pl.when(i >= E - 2)
        def _():
            n0 = (i - (E - 3)) * 2 * PB
            for q in range(PB):
                start_w2(n0 + q)
        return carry

    lax.fori_loop(1, E, up_step, 0)

    def chunk(c, carry):
        def cold_down(t):
            e = (t % E + HOT_ID) % E
            o = jnp.dot(xs[e, :, 0:FF], wbuf[w2_slot(t)], preferred_element_type=F32).astype(BF16)
            ob[:, pl.ds(pl.multiple_of(e * SLOTS, SLOTS), SLOTS), :] = o.reshape(4, SLOTS, CW)

        wait_w2(c * E)

        @pl.when(me == 0)
        def _():
            def hot_down(s, carry2):
                z = zh[pl.ds(2 * s, 2)].reshape(2 * T, FF)
                o = jnp.dot(z, wbuf[w2_slot(c * E)], preferred_element_type=F32).astype(BF16)
                for q in range(2):
                    zhot[2 * s + q] = hgc[2 * s + q] * o[q * T:(q + 1) * T].astype(F32)
                return carry2

            lax.fori_loop(0, 2, hot_down, 0)

        def down(i, carry2):
            t0 = c * E + i * G2

            @pl.when(i > 0)
            def _():
                wait_w2(t0)

            for q in range(1, G2):
                wait_w2(t0 + q)
            for q in range(G2):
                cold_down(t0 + q)
            for p in range(0, G2, PB):
                @pl.when(t0 + N2 + p < NC * E)
                def _():
                    for q in range(PB):
                        start_w2(t0 + N2 + p + q)
            return carry2

        lax.fori_loop(0, E // G2, down, 0)

        def combine(s):
            r = jnp.dot(cm[s], ob[s], preferred_element_type=F32)
            return (r[0:T] + r[T:2 * T]) + r[2 * T:3 * T] + zhot[s]

        p = c % 2
        d_cp = remote(sdiag.at[p], rdiag.at[c], dg_send.at[p], dg_recv.at[c], sib)
        s_cp = remote(ssib.at[p], rsib.at[c], sb_send.at[p], sb_recv.at[c], sib)
        x_cp = remote(scpt.at[c], rcpt.at[c], cp_send.at[c], cp_recv.at[c], cpt)

        @pl.when(c >= 2)
        def _():
            d_cp.wait_send()
            s_cp.wait_send()

        sdiag[p] = combine(3)
        d_cp.start()
        ssib[p] = combine(1)
        s_cp.start()
        scpt[c] = combine(2)
        own[c] = combine(0)
        d_cp.wait_recv()
        scpt[c] = scpt[c] + rdiag[c]
        x_cp.start()
        return carry

    zhot[...] = jnp.zeros_like(zhot)
    lax.fori_loop(0, NC, chunk, 0)

    for c in range(NC):
        cs = slice(c * CW, c * CW + CW)
        remote(ssib.at[0], rsib.at[c], sb_send.at[0], sb_recv.at[c], sib).wait_recv()
        remote(scpt.at[c], rcpt.at[c], cp_send.at[c], cp_recv.at[c], cpt).wait_recv()
        y_ref[:, cs] = (own[c] + rsib[c] + rcpt[c]).astype(BF16)

    m_sib.wait_send()
    m_cpt.wait_send()
    m_fwd.wait_send()
    for i in range(2):
        u_sib[i].wait_send()
    for k in range(NU):
        u_cpt(k).wait_send()
        u_fwd(k).wait_send()
    for p in range(2):
        remote(sdiag.at[p], rdiag.at[p], dg_send.at[p], dg_recv.at[p], sib).wait_send()
        remote(ssib.at[p], rsib.at[p], sb_send.at[p], sb_recv.at[p], sib).wait_send()
    for c in range(NC):
        remote(scpt.at[c], rcpt.at[c], cp_send.at[c], cp_recv.at[c], cpt).wait_send()


def _moe(q, k, v, x, wo, ln2, meta, w1, w3, w2, KC, DH):
    T, D = x.shape
    E, _, FF = w1.shape
    CW = 256
    NC = D // CW
    R = E * SLOTS
    dma = pltpu.SemaphoreType.DMA
    vm = pl.BlockSpec(memory_space=pltpu.VMEM)
    any_spec = pl.BlockSpec(memory_space=pl.ANY)
    part = pltpu.VMEM((NC, T, CW), F32)
    flops = 6 * D * FF * (E * 4 * SLOTS + T)
    return pl.pallas_call(
        functools.partial(_moe_kernel, KC, CW, DH),
        out_shape=jax.ShapeDtypeStruct((T, D), BF16),
        in_specs=[any_spec] * 5 + [vm] + [any_spec] * 4,
        out_specs=pl.BlockSpec(memory_space=pltpu.VMEM),
        scratch_shapes=[
            pltpu.VMEM((4, T, D), BF16),
            pltpu.VMEM((4, 16, T), F32),
            pltpu.VMEM((E, 4 * SLOTS, D), BF16),
            pltpu.VMEM((4 * SLOTS, FF), BF16),
            pltpu.VMEM((4, T, FF), BF16),
            pltpu.VMEM((NW, D, FF), BF16),
            pltpu.VMEM((4, R, CW), BF16),
            pltpu.VMEM((4, 3 * T, R), BF16),
            pltpu.VMEM((4, R, T), BF16),
            pltpu.VMEM((4, T, 1), F32),
            pltpu.VMEM((4, T, CW), F32),
            pltpu.VMEM((2, T, CW), F32),
            pltpu.VMEM((2, T, CW), F32),
            part, part, part, part, part,
            dma((5,)), dma((3, 2)), dma((NW,)), dma((NW * 4,)),
            dma((3,)), dma((3,)),
            dma((NU,)), dma((NU,)), dma((NU,)), dma((NU,)),
            dma((2,)), dma((2,)),
            dma((2,)), dma((NC,)), dma((2,)), dma((NC,)), dma((NC,)), dma((NC,)),
        ],
        compiler_params=pltpu.CompilerParams(
            collective_id=0, has_side_effects=True, vmem_limit_bytes=67000000),
        cost_estimate=pl.CostEstimate(flops=flops, bytes_accessed=6 * E * D * FF, transcendentals=0),
        name='moe',
    )(q, k, v, x, wo.reshape(D, D), ln2.reshape(1, D), meta, w1, w3, w2)


def solution(mesh):
    def local(x, idx, g, hot_tok, hot_g, ln1, wq, wk, wv, wo, ln2, w1, w3, w2):
        n_exp = w1.shape[0] * mesh.shape['expert']
        v, k, q, meta = _qkv(x, ln1, wq, wk, wv, idx, g, hot_tok, hot_g, n_exp)
        return _moe(q, k, v, x, wo, ln2, meta, w1, w3, w2, idx.shape[1], wq.shape[2])

    tk = ('data', 'expert')
    rep3 = P(None, None, None)
    exp3 = P('expert', None, None)
    return jax.shard_map(
        local, mesh=mesh,
        in_specs=(P(tk, None), P(tk, None), P(tk, None), P(tk), P(tk), P(None),
                  rep3, rep3, rep3, rep3, P(None), exp3, exp3, exp3),
        out_specs=P(tk, None), check_vma=False)
```
